8 devices in a mesh: dp: 1 (over z), ep: 8 (over y, x, core).
Axes of the slice: x: 2, y: 2, z: 1, core: 2. Of those that a mesh axis runs over, the one named last changes fastest.
Arguments:
- x_in: bfloat16 [384, 2048], P(('dp', 'ep'))
- topk_idx: int32 [384, 6], P(('dp', 'ep'))
- topk_w: float32 [384, 6], P(('dp', 'ep'))
- w_up: bfloat16 [64, 2048, 1408], P('ep')
- w_down: bfloat16 [64, 1408, 2048], P('ep')
Outputs:
- output: bfloat16 [384, 2048], P(('dp', 'ep'))
All inputs are finite; a program needn't handle non-finite values.
Results may differ from the reference program's by a relative error of at most 0.001.
Values are sent between devices in bfloat16 or wider.
A program may use at most 1 GiB of HBM per device.

```python
import jax
import jax.numpy as jnp
from jax import lax

TOK_DEV = 48
GROUP_SIZE = 8
D_MODEL = 2048
D_FF = 1408
EXPERTS = 64
TOP_K = 6
TOKENS = TOK_DEV * GROUP_SIZE
PAIRS = TOKENS * TOP_K
ROW_WINDOW = min(64, TOKENS)


def draw_routing(route_key):
    key_perm, key_rank, key_start, key_roll = jax.random.split(route_key, 4)
    expert_order = jax.random.permutation(key_perm, EXPERTS).astype(jnp.int32)
    hot_pair = expert_order[:2]
    cold_cycle = expert_order[2:]
    cold_count = EXPERTS - 2
    ranks = jax.vmap(lambda one_key: jax.random.permutation(one_key, TOK_DEV))(jax.random.split(key_rank, GROUP_SIZE)).astype(jnp.int32)
    device_index = jnp.arange(GROUP_SIZE, dtype=jnp.int32)[:, None]
    cold_start = jax.random.randint(key_start, (), 0, cold_count, dtype=jnp.int32)
    cold_base = cold_start + (device_index * TOK_DEV + ranks) * (TOP_K - 1)
    cold_steps = jnp.arange(TOP_K - 1, dtype=jnp.int32)
    cold_ids = cold_cycle[(cold_base[:, :, None] + cold_steps) % cold_count]
    hot_ids = hot_pair[ranks % 2]
    picks = jnp.concatenate([hot_ids[:, :, None], cold_ids], axis=2).reshape(TOKENS, TOP_K)
    shifts = jax.random.randint(key_roll, (TOKENS, 1), 0, TOP_K, dtype=jnp.int32)
    slot_order = (jnp.arange(TOP_K, dtype=jnp.int32)[None, :] + shifts) % TOP_K
    return jnp.take_along_axis(picks, slot_order, axis=1)


def setup_inputs(seed: int = 0, part: int = 0) -> dict:
    part_key = jax.random.fold_in(jax.random.key(seed), part)
    key_x, key_route, key_gate = jax.random.split(part_key, 3)
    key_up, key_down = jax.random.split(jax.random.key(seed + 7919), 2)
    x_in = jax.random.normal(key_x, (TOKENS, D_MODEL), jnp.float32).astype(jnp.bfloat16)
    topk_idx = draw_routing(key_route)
    topk_w = jax.random.uniform(key_gate, (TOKENS, TOP_K), jnp.float32, 0.2, 1.0)
    w_up = lax.map(lambda one_key: (jax.random.normal(one_key, (D_MODEL, D_FF), jnp.float32) * D_MODEL ** -0.5).astype(jnp.bfloat16), jax.random.split(key_up, EXPERTS))
    w_down = lax.map(lambda one_key: (jax.random.normal(one_key, (D_FF, D_MODEL), jnp.float32) * D_FF ** -0.5).astype(jnp.bfloat16), jax.random.split(key_down, EXPERTS))
    return {'x_in': x_in, 'topk_idx': topk_idx, 'topk_w': topk_w, 'w_up': w_up, 'w_down': w_down}


def reference(x_in, topk_idx, topk_w, w_up, w_down):
    flat_ids = topk_idx.reshape(PAIRS)
    order = jnp.argsort(flat_ids, stable=True)
    pad_rows = jnp.zeros((ROW_WINDOW, D_MODEL), x_in.dtype)
    sorted_rows = jnp.concatenate([x_in[order // TOP_K], pad_rows], axis=0)
    counts = jnp.bincount(flat_ids, length=EXPERTS)
    starts = jnp.cumsum(counts) - counts

    def expert_step(expert, results):
        up_mat = w_up[expert]
        down_mat = w_down[expert]

        def window_step(window, acc_rows):
            base = starts[expert] + window * ROW_WINDOW
            rows = lax.dynamic_slice(sorted_rows, (base, 0), (ROW_WINDOW, D_MODEL))
            hidden = jax.nn.gelu(jnp.dot(rows, up_mat, preferred_element_type=jnp.float32), approximate=True).astype(jnp.bfloat16)
            result = jnp.dot(hidden, down_mat, preferred_element_type=jnp.float32).astype(jnp.bfloat16)
            valid = window * ROW_WINDOW + jnp.arange(ROW_WINDOW) < counts[expert]
            current = lax.dynamic_slice(acc_rows, (base, 0), (ROW_WINDOW, D_MODEL))
            return lax.dynamic_update_slice(acc_rows, jnp.where(valid[:, None], result, current), (base, 0))

        windows = (counts[expert] + ROW_WINDOW - 1) // ROW_WINDOW
        return lax.fori_loop(0, windows, window_step, results)

    results = jnp.zeros((PAIRS + ROW_WINDOW, D_MODEL), x_in.dtype)
    results = lax.fori_loop(0, EXPERTS, expert_step, results)
    pair_out = results[jnp.argsort(order)].reshape(TOKENS, TOP_K, D_MODEL)
    mixed = jnp.sum(topk_w[:, :, None] * pair_out.astype(jnp.float32), axis=1)
    return mixed.astype(jnp.bfloat16)
```

```python
import functools

import jax
import jax.numpy as jnp
from jax import lax
from jax.experimental import pallas as pl
from jax.experimental.pallas import tpu as pltpu
from jax.sharding import PartitionSpec as P

MESH = pl.DeviceIdType.MESH
F32 = jnp.float32
BF16 = jnp.bfloat16

UP_SLOTS = 3
DOWN_SLOTS = 4
COLS = 256


def gelu(z):
    inner = 0.7978845608028654 * (z + 0.044715 * (z * z * z))
    return 0.5 * z * (1.0 + jnp.tanh(inner))


def moe_kernel(dims, x_hbm, ids_hbm, gates_hbm, up_hbm, down_hbm, out_ref,
               up_buf, down_buf, ids_v, gates_v, x_all, meta_all, slots, hidden, mix, expert_out,
               part_own, part_send, part_recv, part_in,
               up_sem, down_sem, in_sem, disp_send, disp_recv, fwd_send, fwd_recv,
               pair_send, pair_recv, red_send, red_recv):
    tok, top_n, dim, ff, n_exp, cap = dims
    pair = 2 * tok
    per_exp = 2 * cap
    lanes_n = n_exp * per_exp
    n_blk = dim // COLS
    dp = lax.axis_index('dp')
    me = lax.axis_index('ep')
    core = lax.rem(me, 2)
    chip = me // 2
    cx = lax.rem(chip, 2)
    cy = chip // 2

    def dev(rel, other_core):
        xx = 1 - cx if rel % 2 else cx
        yy = 1 - cy if rel // 2 else cy
        cc = 1 - core if other_core else core
        return (dp, (yy * 2 + xx) * 2 + cc)

    partner = dev(0, True)

    copy_x = pltpu.make_async_copy(x_hbm, x_all.at[0, pl.ds(0, tok)], in_sem.at[0])
    copy_ids = pltpu.make_async_copy(ids_hbm, ids_v, in_sem.at[1])
    copy_gates = pltpu.make_async_copy(gates_hbm, gates_v, in_sem.at[2])
    copy_ids.start()
    copy_gates.start()
    copy_x.start()

    def up_copy(e, slot):
        return pltpu.make_async_copy(up_hbm.at[e], up_buf.at[slot], up_sem.at[slot])

    def down_copy(b, slot):
        return pltpu.make_async_copy(
            down_hbm.at[:, :, pl.ds(b * COLS, COLS)], down_buf.at[slot], down_sem.at[slot])

    for s in range(UP_SLOTS):
        up_copy(s, s).start()
    for s in range(DOWN_SLOTS):
        down_copy(s, s).start()

    barrier = pltpu.get_barrier_semaphore()
    pl.semaphore_signal(barrier, inc=1, device_id=partner, device_id_type=MESH)
    for rel in (1, 2, 3):
        pl.semaphore_signal(barrier, inc=1, device_id=dev(rel, False), device_id_type=MESH)

    copy_ids.wait()
    copy_gates.wait()
    lane = lax.broadcasted_iota(jnp.int32, (tok, 128), 1)
    chosen = jnp.zeros((tok, 128), F32)
    dense_gate = jnp.zeros((tok, 128), F32)
    for j in range(top_n):
        id_j = ids_v[:, j:j + 1]
        w_j = gates_v[:, j:j + 1]
        chosen = jnp.where(lane == id_j, 1.0, chosen)
        dense_gate = jnp.where(lane == id_j + 64, w_j, dense_gate)
    row_i = lax.broadcasted_iota(jnp.int32, (tok, tok), 0)
    col_i = lax.broadcasted_iota(jnp.int32, (tok, tok), 1)
    lower = jnp.where(col_i < row_i, 1.0, 0.0).astype(BF16)
    rank = jnp.dot(lower, chosen.astype(BF16), preferred_element_type=F32)
    meta_all[0, 0:tok, :] = jnp.where(lane < 64, jnp.where(chosen > 0.5, rank, -1.0), dense_gate)
    copy_x.wait()

    pl.semaphore_wait(barrier, 4)

    def dispatch(rel, what):
        ref = x_all if what == 0 else meta_all
        return pltpu.make_async_remote_copy(
            src_ref=ref.at[0, pl.ds(0, tok)], dst_ref=ref.at[rel, pl.ds(0, tok)],
            send_sem=disp_send.at[what, rel], recv_sem=disp_recv.at[what, rel],
            device_id=dev(rel, False), device_id_type=MESH)

    def forward(rel, what):
        ref = x_all if what == 0 else meta_all
        return pltpu.make_async_remote_copy(
            src_ref=ref.at[rel, pl.ds(0, tok)], dst_ref=ref.at[rel, pl.ds(tok, tok)],
            send_sem=fwd_send.at[what, rel], recv_sem=fwd_recv.at[what, rel],
            device_id=partner, device_id_type=MESH)

    for rel in (3, 1, 2):
        dispatch(rel, 1).start()
        dispatch(rel, 0).start()
    forward(0, 1).start()
    forward(0, 0).start()

    e_row = lax.broadcasted_iota(jnp.int32, (128, lanes_n), 0)
    e_col = lax.broadcasted_iota(jnp.int32, (128, lanes_n), 1)
    k_rank = (e_row - n_exp * me) * per_exp
    k_gate = k_rank - 64 * per_exp
    pick_rank = jnp.where((e_col >= k_rank) & (e_col < k_rank + per_exp), 1.0, 0.0).astype(BF16)
    pick_gate = jnp.where((e_col >= k_gate) & (e_col < k_gate + per_exp), 1.0, 0.0).astype(BF16)
    slot_f = lax.broadcasted_iota(jnp.int32, (pair, lanes_n), 1).astype(F32)
    tok_i = lax.broadcasted_iota(jnp.int32, (pair, lanes_n), 0)
    seg = jnp.floor((slot_f + 0.5) * (1.0 / cap))
    want = slot_f - cap * seg
    half = seg - 2.0 * jnp.floor((seg + 0.5) * 0.5)
    own_half = jnp.where(tok_i >= tok, 1.0, 0.0)
    want = jnp.where(half == own_half, want, -2.0)

    def place(rel):
        meta = meta_all[rel]
        g1 = meta.astype(BF16)
        left = meta - g1.astype(F32)
        g2 = left.astype(BF16)
        g3 = (left - g2.astype(F32)).astype(BF16)
        rank_e = jnp.dot(g1, pick_rank, preferred_element_type=F32)
        hit = rank_e == want
        for i, g in enumerate((g1, g2, g3)):
            g_e = jnp.dot(g, pick_gate, preferred_element_type=F32)
            mix[rel, i * pair:(i + 1) * pair, :] = jnp.where(hit, g_e, 0.0).astype(BF16)
        one_hot = jnp.where(hit, 1.0, 0.0).astype(BF16)
        step = 512
        for c in range(dim // step):
            rows = lax.dot_general(one_hot, x_all[rel, :, c * step:(c + 1) * step],
                                   (((0,), (0,)), ((), ())), preferred_element_type=F32).astype(BF16)
            for e in range(n_exp):
                slots[e, rel * per_exp:(rel + 1) * per_exp, c * step:(c + 1) * step] = (
                    rows[e * per_exp:(e + 1) * per_exp])

    forward(0, 1).wait_recv()
    forward(0, 0).wait_recv()
    place(0)
    for rel in (1, 2, 3):
        dispatch(rel, 1).wait_recv()
        forward(rel, 1).start()
        dispatch(rel, 0).wait_recv()
        forward(rel, 0).start()
    for rel in (1, 2, 3):
        forward(rel, 1).wait_recv()
        forward(rel, 0).wait_recv()
        place(rel)

    def up_step(e, carry):
        slot = lax.rem(e, UP_SLOTS)
        up_copy(e, slot).wait()
        base = 0
        while base < ff:
            width = min(512, ff - base)
            z = jnp.dot(slots[e], up_buf[slot, :, base:base + width], preferred_element_type=F32)
            hidden[e, :, base:base + width] = gelu(z).astype(BF16)
            base += width

        @pl.when(e + UP_SLOTS < n_exp)
        def _():
            up_copy(e + UP_SLOTS, slot).start()
        return carry

    lax.fori_loop(0, n_exp, up_step, 0)

    def pair_copy(b):
        return pltpu.make_async_remote_copy(
            src_ref=part_send.at[b], dst_ref=part_recv.at[b],
            send_sem=pair_send.at[b], recv_sem=pair_recv.at[b],
            device_id=partner, device_id_type=MESH)

    def reduce_copy(b, rel):
        return pltpu.make_async_remote_copy(
            src_ref=part_own.at[b, rel], dst_ref=part_in.at[b, rel - 1],
            send_sem=red_send.at[b, rel - 1], recv_sem=red_recv.at[b, rel - 1],
            device_id=dev(rel, False), device_id_type=MESH)

    def reduce_block(b):
        pair_copy(b).wait_recv()
        part_own[b] = part_own[b] + part_recv[b]
        for rel in (3, 1, 2):
            reduce_copy(b, rel).start()

    def down_step(b, carry):
        slot = lax.rem(b, DOWN_SLOTS)
        down_copy(b, slot).wait()
        for e in range(n_exp):
            o = jnp.dot(hidden[e], down_buf[slot, e], preferred_element_type=F32).astype(BF16)
            for rel in range(4):
                expert_out[rel, e * per_exp:(e + 1) * per_exp, :] = o[rel * per_exp:(rel + 1) * per_exp]

        @pl.when(b + DOWN_SLOTS < n_blk)
        def _():
            down_copy(b + DOWN_SLOTS, slot).start()

        for rel in range(4):
            y3 = jnp.dot(mix[rel], expert_out[rel], preferred_element_type=F32)
            y = y3[0:pair] + (y3[pair:2 * pair] + y3[2 * pair:3 * pair])
            part_own[b, rel] = y[0:tok]
            part_send[b, rel] = y[tok:pair]
        pair_copy(b).start()

        @pl.when(b > 0)
        def _():
            reduce_block(b - 1)
        return carry

    lax.fori_loop(0, n_blk, down_step, 0)
    reduce_block(n_blk - 1)

    def finish(b, carry):
        total = part_own[b, 0]
        for rel in (1, 2, 3):
            reduce_copy(b, rel).wait_recv()
            total = total + part_in[b, rel - 1]
        out_ref[:, pl.ds(pl.multiple_of(b * COLS, COLS), COLS)] = total.astype(BF16)
        return carry

    lax.fori_loop(0, n_blk, finish, 0)

    for what in (0, 1):
        for rel in (1, 2, 3):
            dispatch(rel, what).wait_send()
        for rel in range(4):
            forward(rel, what).wait_send()

    def drain(b, carry):
        pair_copy(b).wait_send()
        for rel in (1, 2, 3):
            reduce_copy(b, rel).wait_send()
        return carry

    lax.fori_loop(0, n_blk, drain, 0)


def solution(mesh):
    token_spec = P(('dp', 'ep'), None)
    expert_spec = P('ep', None, None)

    def local_layer(x_loc, ids_loc, gates_loc, w_up, w_down):
        tok, top_n = ids_loc.shape
        dim = x_loc.shape[1]
        n_exp, _, ff = w_up.shape
        cap = tok // 2
        pair = 2 * tok
        lanes_n = n_exp * 2 * cap
        n_blk = dim // COLS
        rows = 8 * cap
        dims = (tok, top_n, dim, ff, n_exp, cap)
        dma = pltpu.SemaphoreType.DMA
        hbm = pl.BlockSpec(memory_space=pl.ANY)
        return pl.pallas_call(
            functools.partial(moe_kernel, dims),
            out_shape=jax.ShapeDtypeStruct((tok, dim), BF16),
            in_specs=[hbm] * 5,
            out_specs=pl.BlockSpec(memory_space=pltpu.VMEM),
            scratch_shapes=[
                pltpu.VMEM((UP_SLOTS, dim, ff), BF16),
                pltpu.VMEM((DOWN_SLOTS, n_exp, ff, COLS), BF16),
                pltpu.VMEM((tok, top_n), jnp.int32),
                pltpu.VMEM((tok, top_n), F32),
                pltpu.VMEM((4, pair, dim), BF16),
                pltpu.VMEM((4, pair, 128), F32),
                pltpu.VMEM((n_exp, rows, dim), BF16),
                pltpu.VMEM((n_exp, rows, ff), BF16),
                pltpu.VMEM((4, 3 * pair, lanes_n), BF16),
                pltpu.VMEM((4, lanes_n, COLS), BF16),
                pltpu.VMEM((n_blk, 4, tok, COLS), F32),
                pltpu.VMEM((n_blk, 4, tok, COLS), F32),
                pltpu.VMEM((n_blk, 4, tok, COLS), F32),
                pltpu.VMEM((n_blk, 3, tok, COLS), F32),
                dma((UP_SLOTS,)), dma((DOWN_SLOTS,)), dma((3,)),
                dma((2, 4)), dma((2, 4)), dma((2, 4)), dma((2, 4)),
                dma((n_blk,)), dma((n_blk,)), dma((n_blk, 3)), dma((n_blk, 3)),
            ],
            compiler_params=pltpu.CompilerParams(
                collective_id=0, has_side_effects=True, vmem_limit_bytes=67043328),
            name='moe_layer',
        )(x_loc, ids_loc, gates_loc, w_up, w_down)

    return jax.shard_map(local_layer, mesh=mesh, in_specs=(token_spec, token_spec, token_spec, expert_spec, expert_spec),
                         out_specs=token_spec, check_vma=False)
```

```python
import functools

import jax
import jax.numpy as jnp
from jax import lax
from jax.experimental import pallas as pl
from jax.experimental.pallas import tpu as pltpu
from jax.sharding import PartitionSpec as P

MESH = pl.DeviceIdType.MESH
F32 = jnp.float32
BF16 = jnp.bfloat16

UP_SLOTS = 6
EARLY = 4
RING = UP_SLOTS // 2
PER_SLOT = 5
COLS = 256
HALF = COLS // 2
CHUNKS = 4


def gelu(z):
    inner = 0.7978845608028654 * (z + 0.044715 * (z * z * z))
    return 0.5 * z * (1.0 + jnp.tanh(inner))


def moe_kernel(dims, x_hbm, ids_hbm, gates_hbm, up_hbm, down_hbm, out_hbm,
               up_buf, first_buf, out_v, ids_v, gates_v, x_all, meta_all, one_hot, slots, acc, hidden, mix, expert_out,
               part_own, part_send, part_recv, in_x1, in_y1, in_x2, in_y2, in_last,
               up_sem, first_sem, down_sem, out_sem, in_sem, meta_send, meta_recv, tok_send, tok_recv, diag_send, diag_recv,
               mpair_send, mpair_recv, tpair_send, tpair_recv,
               pair_send, pair_recv, red_send, red_recv, last_send, last_recv):
    tok, top_n, dim, ff, n_exp, cap = dims
    pair = 2 * tok
    per_exp = 2 * cap
    lanes_n = n_exp * per_exp
    n_blk = dim // COLS
    chunk = dim // CHUNKS
    dp = lax.axis_index('dp')
    me = lax.axis_index('ep')
    core = lax.rem(me, 2)
    chip = me // 2
    cx = lax.rem(chip, 2)
    cy = chip // 2

    def dev(rel, other_core):
        xx = 1 - cx if rel % 2 else cx
        yy = 1 - cy if rel // 2 else cy
        cc = 1 - core if other_core else core
        return (dp, (yy * 2 + xx) * 2 + cc)

    partner = dev(0, True)

    barrier = pltpu.get_barrier_semaphore()
    for rel in (3, 1, 2):
        pl.semaphore_signal(barrier, inc=1, device_id=dev(rel, False), device_id_type=MESH)
    pl.semaphore_signal(barrier, inc=1, device_id=partner, device_id_type=MESH)

    copy_x = pltpu.make_async_copy(x_hbm, x_all.at[0, pl.ds(0, tok)], in_sem.at[0])
    copy_ids = pltpu.make_async_copy(ids_hbm, ids_v, in_sem.at[1])
    copy_gates = pltpu.make_async_copy(gates_hbm, gates_v, in_sem.at[2])
    copy_x.start()
    copy_ids.start()
    copy_gates.start()

    def up_copy(e):
        slot = lax.rem(e, UP_SLOTS)
        return pltpu.make_async_copy(up_hbm.at[e], up_buf.at[slot], up_sem.at[slot])

    first_copy = pltpu.make_async_copy(down_hbm.at[:, :, pl.ds(0, COLS)], first_buf, first_sem.at[0])

    def down_place(b, e):
        return 2 * lax.rem(b, RING) + e // PER_SLOT, (e % PER_SLOT) * COLS

    def down_copy(b, e):
        slot, col = down_place(b, e)
        return pltpu.make_async_copy(
            down_hbm.at[e, :, pl.ds(pl.multiple_of(b * COLS, COLS), COLS)], up_buf.at[slot, pl.ds(0, ff), pl.ds(col, COLS)],
            down_sem.at[lax.rem(b, RING), e])

    def down_start(b):
        for e in range(n_exp):
            down_copy(b, e).start()

    copy_ids.wait()
    copy_gates.wait()
    copy_x.wait()
    for e in range(UP_SLOTS):
        up_copy(e).start()
    first_copy.start()

    def remote(src, dst, send, recv, to):
        return pltpu.make_async_remote_copy(
            src_ref=src, dst_ref=dst, send_sem=send, recv_sem=recv, device_id=to, device_id_type=MESH)

    def meta_out(rel):
        return remote(meta_all.at[0, pl.ds(0, tok)], meta_all.at[rel, pl.ds(0, tok)],
                      meta_send.at[rel], meta_recv.at[rel], dev(rel, False))

    def meta_pair(rel):
        return remote(meta_all.at[rel, pl.ds(0, tok)], meta_all.at[rel, pl.ds(tok, tok)],
                      mpair_send.at[rel], mpair_recv.at[rel], partner)

    def tok_out(rel, c):
        cols = pl.ds(c * chunk, chunk)
        return remote(x_all.at[0, pl.ds(0, tok), cols], x_all.at[rel, pl.ds(0, tok), cols],
                      tok_send.at[rel, c], tok_recv.at[rel, c], dev(rel, False))

    def tok_diag(via, c):
        cols = pl.ds(c * chunk + (via - 1) * (chunk // 2), chunk // 2)
        return remote(x_all.at[via, pl.ds(0, tok), cols], x_all.at[3, pl.ds(0, tok), cols],
                      diag_send.at[via, c], diag_recv.at[via, c], dev(3 - via, False))

    def tok_pair(rel, c):
        cols = pl.ds(c * chunk, chunk)
        return remote(x_all.at[rel, pl.ds(0, tok), cols], x_all.at[rel, pl.ds(tok, tok), cols],
                      tpair_send.at[rel, c], tpair_recv.at[rel, c], partner)

    pl.semaphore_wait(barrier, 4)
    tok_out(1, 0).start()
    tok_out(2, 0).start()
    for c in range(CHUNKS):
        tok_pair(0, c).start()

    sub = lax.broadcasted_iota(jnp.int32, (64, tok), 0)
    chosen = jnp.zeros((64, tok), F32)
    dense_gate = jnp.zeros((64, tok), F32)
    for j in range(top_n):
        same = sub == ids_v[j:j + 1, :]
        chosen = jnp.where(same, 1.0, chosen)
        dense_gate = jnp.where(same, gates_v[j:j + 1, :], dense_gate)
    row_i = lax.broadcasted_iota(jnp.int32, (tok, tok), 0)
    col_i = lax.broadcasted_iota(jnp.int32, (tok, tok), 1)
    before = jnp.where(row_i < col_i, 1.0, 0.0).astype(BF16)
    rank = jnp.dot(chosen.astype(BF16), before, preferred_element_type=F32)
    meta_t = jnp.concatenate([jnp.where(chosen > 0.5, rank, -1.0), dense_gate], axis=0)
    meta_all[0, 0:tok, :] = meta_t.T
    for rel in (3, 1, 2):
        meta_out(rel).start()
    meta_pair(0).start()
    for c in (1, 2):
        tok_out(1, c).start()
        tok_out(2, c).start()

    e_row = lax.broadcasted_iota(jnp.int32, (128, lanes_n), 0)
    e_col = lax.broadcasted_iota(jnp.int32, (128, lanes_n), 1)
    k_rank = (e_row - n_exp * me) * per_exp
    k_gate = k_rank - 64 * per_exp
    pick_rank = jnp.where((e_col >= k_rank) & (e_col < k_rank + per_exp), 1.0, 0.0).astype(BF16)
    pick_gate = jnp.where((e_col >= k_gate) & (e_col < k_gate + per_exp), 1.0, 0.0).astype(BF16)
    slot_f = lax.broadcasted_iota(jnp.int32, (pair, lanes_n), 1).astype(F32)
    tok_i = lax.broadcasted_iota(jnp.int32, (pair, lanes_n), 0)
    seg = jnp.floor((slot_f + 0.5) * (1.0 / cap))
    want = slot_f - cap * seg
    half = seg - 2.0 * jnp.floor((seg + 0.5) * 0.5)
    own_half = jnp.where(tok_i >= tok, 1.0, 0.0)
    want = jnp.where(half == own_half, want, -2.0)

    def masks(rels):
        for rel in rels:
            meta_pair(rel).wait_recv()
        for rel in rels:
            meta = meta_all[rel]
            g1 = meta.astype(BF16)
            left = meta - g1.astype(F32)
            g2 = left.astype(BF16)
            g3 = (left - g2.astype(F32)).astype(BF16)
            rank_e = jnp.dot(g1, pick_rank, preferred_element_type=F32)
            hit = rank_e == want
            for i, g in enumerate((g1, g2, g3)):
                g_e = jnp.dot(g, pick_gate, preferred_element_type=F32)
                mix[rel, i * pair:(i + 1) * pair, :] = jnp.where(hit, g_e, 0.0).astype(BF16)
            one_hot[rel] = jnp.where(hit, 1.0, 0.0).astype(BF16)

    def arrived(c):
        for via in (1, 2):
            tok_out(via, c).wait_recv()
            tok_diag(via, c).start()
            tok_pair(via, c).start()

    def diag_arrived(c):
        for via in (1, 2):
            tok_diag(via, c).wait_recv()
        tok_pair(3, c).start()

    def place(rels, cs):
        for c in cs:
            for rel in rels:
                tok_pair(rel, c).wait_recv()
        for c in cs:
            for rel in rels:
                rows = lax.dot_general(one_hot[rel], x_all[rel, :, c * chunk:(c + 1) * chunk],
                                       (((0,), (0,)), ((), ())), preferred_element_type=F32).astype(BF16)
                for e in range(n_exp):
                    slots[e, rel * per_exp:(rel + 1) * per_exp, c * chunk:(c + 1) * chunk] = (
                        rows[e * per_exp:(e + 1) * per_exp])

    def early(e):
        up_copy(e).wait()
        z = jnp.dot(slots[e, 0:per_exp, :], up_buf[e], preferred_element_type=F32)
        hidden[e, 0:per_exp, :] = gelu(z).astype(BF16)

    def late_dot(e, lo, hi):
        return jnp.dot(slots[e, per_exp:, lo:hi], up_buf[e, lo:hi, :], preferred_element_type=F32)

    def work_first():
        for e in range(EARLY):
            acc[e] = late_dot(e, 0, chunk)

    def work_second():
        for e in range(EARLY):
            acc[e] = acc[e] + late_dot(e, chunk, 2 * chunk)

    def work_third(e0, e1):
        for e in range(e0, e1):
            hidden[e, per_exp:, :] = gelu(acc[e] + late_dot(e, 2 * chunk, dim)).astype(BF16)
        for e in range(e0, e1):
            if e + UP_SLOTS < n_exp:
                up_copy(e + UP_SLOTS).start()

    def work_whole(e0, e1):
        for e in range(e0, e1):
            up_copy(e).wait()
        for e in range(e0, e1):
            z = jnp.dot(slots[e], up_buf[e % UP_SLOTS], preferred_element_type=F32)
            hidden[e] = gelu(z).astype(BF16)

    masks((0,))
    place((0,), range(CHUNKS))
    early(0)
    early(1)
    arrived(0)
    tok_out(1, 3).start()
    tok_out(2, 3).start()
    early(2)
    for rel in (1, 2, 3):
        meta_out(rel).wait_recv()
        meta_pair(rel).start()
    arrived(1)
    early(3)
    arrived(2)
    masks((1, 2, 3))
    diag_arrived(0)
    place((1, 2), (0,))
    arrived(3)
    diag_arrived(1)
    place((3,), (0,))
    work_first()
    diag_arrived(2)
    diag_arrived(3)
    place((1, 2, 3), (1,))
    work_second()
    place((1, 2, 3), (2, 3))
    work_third(0, 2)
    work_third(2, 4)
    down_start(1)
    work_whole(4, 6)
    down_start(2)
    work_whole(6, 8)
    down_start(3)

    def pair_copy(b):
        return remote(part_send.at[b], part_recv.at[b], pair_send.at[b], pair_recv.at[b], partner)

    lo, hi = pl.ds(0, HALF), pl.ds(HALF, HALF)
    everyone = pl.ds(0, 2)

    def first_x(b):
        return remote(part_own.at[b, everyone, 1, :, lo], in_x1.at[b], red_send.at[b, 0], red_recv.at[b, 0], dev(1, False))

    def first_y(b):
        return remote(part_own.at[b, 1, everyone, :, hi], in_y1.at[b], red_send.at[b, 1], red_recv.at[b, 1], dev(2, False))

    def second_y(b):
        return remote(part_own.at[b, 1, 0, :, lo], in_y2.at[b], red_send.at[b, 2], red_recv.at[b, 2], dev(2, False))

    def second_x(b):
        return remote(part_own.at[b, 0, 1, :, hi], in_x2.at[b], red_send.at[b, 3], red_recv.at[b, 3], dev(1, False))

    def stage_one(b):
        pair_copy(b).wait_recv()
        part_own[b] = part_own[b] + part_recv[b]
        first_x(b).start()
        first_y(b).start()

    def stage_two(b):
        first_x(b).wait_recv()
        part_own[b, 1, 0, :, 0:HALF] = part_own[b, 1, 0, :, 0:HALF] + in_x1[b, 1]
        second_y(b).start()
        first_y(b).wait_recv()
        part_own[b, 0, 1, :, HALF:COLS] = part_own[b, 0, 1, :, HALF:COLS] + in_y1[b, 1]
        second_x(b).start()

    def down_dot(e, weights):
        o = jnp.dot(hidden[e], weights, preferred_element_type=F32).astype(BF16)
        for rel in range(4):
            expert_out[rel, e * per_exp:(e + 1) * per_exp, :] = o[rel * per_exp:(rel + 1) * per_exp]

    def combine(b):
        for rel in range(4):
            y3 = jnp.dot(mix[rel], expert_out[rel], preferred_element_type=F32)
            y = y3[0:pair] + (y3[pair:2 * pair] + y3[2 * pair:3 * pair])
            part_own[b, rel // 2, rel % 2] = y[0:tok]
            part_send[b, rel // 2, rel % 2] = y[tok:pair]
        pair_copy(b).start()

    def down_first():
        first_copy.wait()
        for e in range(n_exp):
            down_dot(e, first_buf[e])
        combine(0)

    def down_step(b, carry):
        for e in range(n_exp):
            down_copy(b, e).wait()
        for e in range(n_exp):
            slot, col = down_place(b, e)
            down_dot(e, up_buf[slot, 0:ff, col:col + COLS])

        @pl.when(b + RING < n_blk)
        def _():
            down_start(b + RING)

        stage_one(b - 1)

        @pl.when(b > 2)
        def _():
            stage_two(b - 3)

        combine(b)
        return carry

    def out_copy(b):
        cols = pl.ds(pl.multiple_of(b * COLS, COLS), COLS)
        return pltpu.make_async_copy(out_v.at[b], out_hbm.at[:, cols], out_sem.at[b])

    def finish(b, carry):
        second_y(b).wait_recv()
        left = part_own[b, 0, 0, :, 0:HALF] + in_x1[b, 0] + in_y2[b]
        out_v[b, :, 0:HALF] = left.astype(BF16)
        second_x(b).wait_recv()
        right = part_own[b, 0, 0, :, HALF:COLS] + in_y1[b, 0] + in_x2[b]
        out_v[b, :, HALF:COLS] = right.astype(BF16)
        out_copy(b).start()
        return carry

    last = n_blk - 1

    def last_copy(rel):
        return remote(part_own.at[last, rel // 2, rel % 2], in_last.at[rel - 1],
                      last_send.at[rel - 1], last_recv.at[rel - 1], dev(rel, False))

    down_first()
    lax.fori_loop(1, n_blk, down_step, 0)
    stage_two(last - 2)
    lax.fori_loop(0, last - 4, finish, 0)
    pair_copy(last).wait_recv()
    part_own[last] = part_own[last] + part_recv[last]
    for rel in (3, 1, 2):
        last_copy(rel).start()
    stage_two(last - 1)
    lax.fori_loop(last - 4, last, finish, 0)
    for rel in (1, 2, 3):
        last_copy(rel).wait_recv()
    total = part_own[last, 0, 0] + in_last[0] + in_last[1] + in_last[2]
    out_v[last] = total.astype(BF16)
    out_copy(last).start()

    for rel in range(4):
        meta_pair(rel).wait_send()
        if rel:
            meta_out(rel).wait_send()
        for c in range(CHUNKS):
            tok_pair(rel, c).wait_send()
            if rel in (1, 2):
                tok_out(rel, c).wait_send()
                tok_diag(rel, c).wait_send()

    for rel in (1, 2, 3):
        last_copy(rel).wait_send()
    pair_copy(last).wait_send()

    def drain(b, carry):
        for copy in (pair_copy, first_x, first_y, second_x, second_y):
            copy(b).wait_send()
        return carry

    lax.fori_loop(0, last, drain, 0)
    def flush(b, carry):
        out_copy(b).wait()
        return carry

    lax.fori_loop(0, n_blk, flush, 0)


def solution(mesh):
    token_spec = P(('dp', 'ep'), None)
    expert_spec = P('ep', None, None)

    def local_layer(x_loc, ids_loc, gates_loc, w_up, w_down):
        tok, top_n = ids_loc.shape
        dim = x_loc.shape[1]
        n_exp, _, ff = w_up.shape
        cap = tok // 2
        pair = 2 * tok
        lanes_n = n_exp * 2 * cap
        n_blk = dim // COLS
        rows = 8 * cap
        dims = (tok, top_n, dim, ff, n_exp, cap)
        dma = pltpu.SemaphoreType.DMA
        hbm = pl.BlockSpec(memory_space=pl.ANY)
        return pl.pallas_call(
            functools.partial(moe_kernel, dims),
            out_shape=jax.ShapeDtypeStruct((tok, dim), BF16),
            in_specs=[hbm] * 5,
            out_specs=hbm,
            scratch_shapes=[
                pltpu.VMEM((UP_SLOTS, dim, ff), BF16),
                pltpu.VMEM((n_exp, ff, COLS), BF16),
                pltpu.VMEM((n_blk, tok, COLS), BF16),
                pltpu.VMEM((top_n, tok), jnp.int32),
                pltpu.VMEM((top_n, tok), F32),
                pltpu.VMEM((4, pair, dim), BF16),
                pltpu.VMEM((4, pair, 128), F32),
                pltpu.VMEM((4, pair, lanes_n), BF16),
                pltpu.VMEM((n_exp, rows, dim), BF16),
                pltpu.VMEM((EARLY, rows - 2 * cap, ff), F32),
                pltpu.VMEM((n_exp, rows, ff), BF16),
                pltpu.VMEM((4, 3 * pair, lanes_n), BF16),
                pltpu.VMEM((4, lanes_n, COLS), BF16),
                pltpu.VMEM((n_blk, 2, 2, tok, COLS), F32),
                pltpu.VMEM((n_blk, 2, 2, tok, COLS), F32),
                pltpu.VMEM((n_blk, 2, 2, tok, COLS), F32),
                pltpu.VMEM((n_blk, 2, tok, HALF), F32),
                pltpu.VMEM((n_blk, 2, tok, HALF), F32),
                pltpu.VMEM((n_blk, tok, HALF), F32),
                pltpu.VMEM((n_blk, tok, HALF), F32),
                pltpu.VMEM((3, tok, COLS), F32),
                dma((UP_SLOTS,)), dma((1,)), dma((RING, n_exp)), dma((n_blk,)), dma((3,)),
                dma((4,)), dma((4,)),
                dma((3, CHUNKS)), dma((3, CHUNKS)), dma((3, CHUNKS)), dma((3, CHUNKS)),
                dma((4,)), dma((4,)), dma((4, CHUNKS)), dma((4, CHUNKS)),
                dma((n_blk,)), dma((n_blk,)), dma((n_blk, 4)), dma((n_blk, 4)),
                dma((3,)), dma((3,)),
            ],
            compiler_params=pltpu.CompilerParams(
                collective_id=0, has_side_effects=True, vmem_limit_bytes=67043328),
            name='moe_layer',
        )(x_loc, ids_loc.T, gates_loc.T, w_up, w_down)

    return jax.shard_map(local_layer, mesh=mesh, in_specs=(token_spec, token_spec, token_spec, expert_spec, expert_spec),
                         out_specs=token_spec, check_vma=False)
```

```python
import functools

import jax
import jax.numpy as jnp
from jax import lax
from jax.experimental import pallas as pl
from jax.experimental.pallas import tpu as pltpu
from jax.sharding import PartitionSpec as P

MESH = pl.DeviceIdType.MESH
F32 = jnp.float32
BF16 = jnp.bfloat16

UP_SLOTS = 6
EARLY = 4
RING = UP_SLOTS // 2
PER_SLOT = 5
COLS = 256
HALF = COLS // 2
CHUNKS = 4


def gelu(z):
    inner = 0.7978845608028654 * (z + 0.044715 * (z * z * z))
    return 0.5 * z * (1.0 + jnp.tanh(inner))


def moe_kernel(dims, x_hbm, ids_hbm, gates_hbm, up_hbm, down_hbm, out_ref,
               up_buf, first_buf, ids_v, gates_v, x_all, meta_all, one_hot, slots, acc, hidden, mix, expert_out,
               part_own, part_send, part_recv, in_x1, in_y1, in_two, in_last,
               up_sem, first_sem, down_sem, in_sem, send_sem, meta_recv, mpair_recv,
               tok_recv, diag_recv, tpair_recv, pair_recv, one_recv, two_recv, last_recv):
    tok, top_n, dim, ff, n_exp, cap = dims
    pair = 2 * tok
    per_exp = 2 * cap
    lanes_n = n_exp * per_exp
    n_blk = dim // COLS
    chunk = dim // CHUNKS
    dp = lax.axis_index('dp')
    me = lax.axis_index('ep')
    core = lax.rem(me, 2)
    chip = me // 2
    cx = lax.rem(chip, 2)
    cy = chip // 2

    def dev(rel, other_core):
        xx = 1 - cx if rel % 2 else cx
        yy = 1 - cy if rel // 2 else cy
        cc = 1 - core if other_core else core
        return (dp, (yy * 2 + xx) * 2 + cc)

    partner = dev(0, True)

    barrier = pltpu.get_barrier_semaphore()
    for rel in (3, 1, 2):
        pl.semaphore_signal(barrier, inc=1, device_id=dev(rel, False), device_id_type=MESH)
    pl.semaphore_signal(barrier, inc=1, device_id=partner, device_id_type=MESH)

    copy_x = pltpu.make_async_copy(x_hbm, x_all.at[0, pl.ds(0, tok)], in_sem.at[0])
    copy_ids = pltpu.make_async_copy(ids_hbm, ids_v, in_sem.at[1])
    copy_gates = pltpu.make_async_copy(gates_hbm, gates_v, in_sem.at[2])
    copy_x.start()
    copy_ids.start()
    copy_gates.start()

    def up_copy(e):
        slot = lax.rem(e, UP_SLOTS)
        return pltpu.make_async_copy(up_hbm.at[e], up_buf.at[slot], up_sem.at[slot])

    first_copy = pltpu.make_async_copy(down_hbm.at[:, :, pl.ds(0, COLS)], first_buf, first_sem.at[0])

    def down_place(b, e):
        return 2 * lax.rem(b, RING) + e // PER_SLOT, (e % PER_SLOT) * COLS

    def down_copy(b, e):
        slot, col = down_place(b, e)
        return pltpu.make_async_copy(
            down_hbm.at[e, :, pl.ds(pl.multiple_of(b * COLS, COLS), COLS)], up_buf.at[slot, pl.ds(0, ff), pl.ds(col, COLS)],
            down_sem.at[lax.rem(b, RING)])

    def down_start(b):
        for e in range(n_exp):
            down_copy(b, e).start()

    def down_wait(b):
        pltpu.make_async_copy(down_hbm.at[:, :, pl.ds(0, COLS)], first_buf, down_sem.at[lax.rem(b, RING)]).wait()

    copy_ids.wait()
    copy_gates.wait()
    copy_x.wait()
    for e in range(UP_SLOTS):
        up_copy(e).start()
    first_copy.start()

    def remote(src, dst, send, recv, to):
        return pltpu.make_async_remote_copy(
            src_ref=src, dst_ref=dst, send_sem=send, recv_sem=recv, device_id=to, device_id_type=MESH)

    meta_sent, tok_sent, pair_sent, one_sent, two_sent, last_sent = (send_sem.at[i] for i in range(6))

    def meta_out(rel):
        return remote(meta_all.at[0, pl.ds(0, tok)], meta_all.at[rel, pl.ds(0, tok)],
                      meta_sent, meta_recv.at[rel - 1], dev(rel, False))

    def meta_pair(rel):
        return remote(meta_all.at[rel, pl.ds(0, tok)], meta_all.at[rel, pl.ds(tok, tok)],
                      meta_sent, mpair_recv.at[min(rel, 1)], partner)

    def tok_out(rel, c):
        cols = pl.ds(c * chunk, chunk)
        return remote(x_all.at[0, pl.ds(0, tok), cols], x_all.at[rel, pl.ds(0, tok), cols],
                      tok_sent, tok_recv.at[rel - 1, c], dev(rel, False))

    def tok_diag(via, c):
        cols = pl.ds(c * chunk + (via - 1) * (chunk // 2), chunk // 2)
        return remote(x_all.at[via, pl.ds(0, tok), cols], x_all.at[3, pl.ds(0, tok), cols],
                      tok_sent, diag_recv.at[c], dev(3 - via, False))

    def tok_pair(rel, c):
        cols = pl.ds(c * chunk, chunk)
        return remote(x_all.at[rel, pl.ds(0, tok), cols], x_all.at[rel, pl.ds(tok, tok), cols],
                      tok_sent, tpair_recv.at[0 if rel == 3 else 1, c], partner)

    own_pair = remote(x_all.at[0, pl.ds(0, tok)], x_all.at[0, pl.ds(tok, tok)], tok_sent, tpair_recv.at[2, 0], partner)

    def landed(ref, sem):
        remote(ref, ref, send_sem.at[0], sem, partner).wait_recv()

    def left(ref, sem):
        remote(ref, ref, sem, tpair_recv.at[0, 0], partner).wait_send()

    pl.semaphore_wait(barrier, 4)
    tok_out(1, 0).start()
    tok_out(2, 0).start()
    own_pair.start()

    sub = lax.broadcasted_iota(jnp.int32, (64, tok), 0)
    chosen = jnp.zeros((64, tok), F32)
    dense_gate = jnp.zeros((64, tok), F32)
    for j in range(top_n):
        same = sub == ids_v[j:j + 1, :]
        chosen = jnp.where(same, 1.0, chosen)
        dense_gate = jnp.where(same, gates_v[j:j + 1, :], dense_gate)
    row_i = lax.broadcasted_iota(jnp.int32, (tok, tok), 0)
    col_i = lax.broadcasted_iota(jnp.int32, (tok, tok), 1)
    before = jnp.where(row_i < col_i, 1.0, 0.0).astype(BF16)
    rank = jnp.dot(chosen.astype(BF16), before, preferred_element_type=F32)
    meta_t = jnp.concatenate([jnp.where(chosen > 0.5, rank, -1.0), dense_gate], axis=0)
    meta_all[0, 0:tok, :] = meta_t.T
    for rel in (3, 1, 2):
        meta_out(rel).start()
    meta_pair(0).start()
    for c in (1, 2):
        tok_out(1, c).start()
        tok_out(2, c).start()

    e_row = lax.broadcasted_iota(jnp.int32, (128, lanes_n), 0)
    e_col = lax.broadcasted_iota(jnp.int32, (128, lanes_n), 1)
    k_rank = (e_row - n_exp * me) * per_exp
    k_gate = k_rank - 64 * per_exp
    pick_rank = jnp.where((e_col >= k_rank) & (e_col < k_rank + per_exp), 1.0, 0.0).astype(BF16)
    pick_gate = jnp.where((e_col >= k_gate) & (e_col < k_gate + per_exp), 1.0, 0.0).astype(BF16)
    slot_f = lax.broadcasted_iota(jnp.int32, (pair, lanes_n), 1).astype(F32)
    tok_i = lax.broadcasted_iota(jnp.int32, (pair, lanes_n), 0)
    seg = jnp.floor((slot_f + 0.5) * (1.0 / cap))
    want = slot_f - cap * seg
    half = seg - 2.0 * jnp.floor((seg + 0.5) * 0.5)
    own_half = jnp.where(tok_i >= tok, 1.0, 0.0)
    want = jnp.where(half == own_half, want, -2.0)

    def masks(rels):
        if rels == (0,):
            meta_pair(0).wait_recv()
        else:
            landed(meta_all.at[pl.ds(1, 3), pl.ds(tok, tok)], mpair_recv.at[1])
        for rel in rels:
            meta = meta_all[rel]
            g1 = meta.astype(BF16)
            rest = meta - g1.astype(F32)
            g2 = rest.astype(BF16)
            g3 = (rest - g2.astype(F32)).astype(BF16)
            rank_e = jnp.dot(g1, pick_rank, preferred_element_type=F32)
            hit = rank_e == want
            for i, g in enumerate((g1, g2, g3)):
                g_e = jnp.dot(g, pick_gate, preferred_element_type=F32)
                mix[rel, i * pair:(i + 1) * pair, :] = jnp.where(hit, g_e, 0.0).astype(BF16)
            one_hot[rel] = jnp.where(hit, 1.0, 0.0).astype(BF16)

    def arrived(c):
        for via in (1, 2):
            tok_out(via, c).wait_recv()
            tok_diag(via, c).start()
            tok_pair(via, c).start()

    def diag_arrived(c):
        cols = pl.ds(c * chunk, chunk)
        landed(x_all.at[3, pl.ds(0, tok), cols], diag_recv.at[c])
        tok_pair(3, c).start()

    def place(rels, cs):
        for c in cs:
            cols = pl.ds(c * chunk, chunk)
            if 0 in rels and c == 0:
                own_pair.wait_recv()
            if 1 in rels:
                landed(x_all.at[pl.ds(1, 2), pl.ds(tok, tok), cols], tpair_recv.at[1, c])
            if 3 in rels:
                landed(x_all.at[3, pl.ds(tok, tok), cols], tpair_recv.at[0, c])
        for c in cs:
            for rel in rels:
                rows = lax.dot_general(one_hot[rel], x_all[rel, :, c * chunk:(c + 1) * chunk],
                                       (((0,), (0,)), ((), ())), preferred_element_type=F32).astype(BF16)
                for e in range(n_exp):
                    slots[e, rel * per_exp:(rel + 1) * per_exp, c * chunk:(c + 1) * chunk] = (
                        rows[e * per_exp:(e + 1) * per_exp])

    def early(e):
        up_copy(e).wait()
        z = jnp.dot(slots[e, 0:per_exp, :], up_buf[e], preferred_element_type=F32)
        hidden[e, 0:per_exp, :] = gelu(z).astype(BF16)

    def late_dot(e, lo, hi):
        return jnp.dot(slots[e, per_exp:, lo:hi], up_buf[e, lo:hi, :], preferred_element_type=F32)

    def work_first():
        for e in range(EARLY):
            acc[e] = late_dot(e, 0, chunk)

    def work_second(e0, e1):
        for e in range(e0, e1):
            acc[e] = acc[e] + late_dot(e, chunk, 2 * chunk)

    def work_third(e0, e1):
        for e in range(e0, e1):
            hidden[e, per_exp:, :] = gelu(acc[e] + late_dot(e, 2 * chunk, dim)).astype(BF16)
        for e in range(e0, e1):
            if e + UP_SLOTS < n_exp:
                up_copy(e + UP_SLOTS).start()

    def work_whole(e0, e1):
        for e in range(e0, e1):
            up_copy(e).wait()
        for e in range(e0, e1):
            z = jnp.dot(slots[e], up_buf[e % UP_SLOTS], preferred_element_type=F32)
            hidden[e] = gelu(z).astype(BF16)

    masks((0,))
    place((0,), range(CHUNKS))
    early(0)
    arrived(0)
    tok_out(1, 3).start()
    tok_out(2, 3).start()
    early(1)
    for rel in (1, 2, 3):
        meta_out(rel).wait_recv()
        meta_pair(rel).start()
    arrived(1)
    early(2)
    arrived(2)
    masks((1, 2, 3))
    diag_arrived(0)
    early(3)
    arrived(3)
    diag_arrived(1)
    place((1, 2), (0,))
    place((3,), (0,))
    work_first()
    diag_arrived(2)
    place((1, 2, 3), (1,))
    work_second(0, 2)
    diag_arrived(3)
    work_second(2, 4)
    place((1, 2, 3), (2,))
    place((1, 2, 3), (3,))
    work_third(0, 2)
    work_third(2, 4)
    down_start(1)
    work_whole(4, 6)
    down_start(2)
    work_whole(6, 8)
    down_start(3)

    def pair_copy(b):
        return remote(part_send.at[b], part_recv.at[b], pair_sent, pair_recv.at[b], partner)

    lo, hi = pl.ds(0, HALF), pl.ds(HALF, HALF)
    everyone = pl.ds(0, 2)

    def first_x(b):
        return remote(part_own.at[b, everyone, 1, :, lo], in_x1.at[b], one_sent, one_recv.at[b, 0], dev(1, False))

    def first_y(b):
        return remote(part_own.at[b, 1, everyone, :, hi], in_y1.at[b], one_sent, one_recv.at[b, 1], dev(2, False))

    def second_y(b):
        return remote(part_own.at[b, 1, 0, :, lo], in_two.at[b, 0], two_sent, two_recv.at[b], dev(2, False))

    def second_x(b):
        return remote(part_own.at[b, 0, 1, :, hi], in_two.at[b, 1], two_sent, two_recv.at[b], dev(1, False))

    def stage_one(b):
        pair_copy(b).wait_recv()
        part_own[b] = part_own[b] + part_recv[b]
        first_x(b).start()
        first_y(b).start()

    def stage_two(b):
        first_x(b).wait_recv()
        part_own[b, 1, 0, :, 0:HALF] = part_own[b, 1, 0, :, 0:HALF] + in_x1[b, 1]
        second_y(b).start()
        first_y(b).wait_recv()
        part_own[b, 0, 1, :, HALF:COLS] = part_own[b, 0, 1, :, HALF:COLS] + in_y1[b, 1]
        second_x(b).start()

    def down_dot(e, weights):
        o = jnp.dot(hidden[e], weights, preferred_element_type=F32).astype(BF16)
        for rel in range(4):
            expert_out[rel, e * per_exp:(e + 1) * per_exp, :] = o[rel * per_exp:(rel + 1) * per_exp]

    def combine(b):
        for rel in range(4):
            y3 = jnp.dot(mix[rel], expert_out[rel], preferred_element_type=F32)
            y = y3[0:pair] + (y3[pair:2 * pair] + y3[2 * pair:3 * pair])
            part_own[b, rel // 2, rel % 2] = y[0:tok]
            part_send[b, rel // 2, rel % 2] = y[tok:pair]
        pair_copy(b).start()

    def down_first():
        first_copy.wait()
        for e in range(n_exp):
            down_dot(e, first_buf[e])
        combine(0)

    def down_step(b, carry):
        down_wait(b)
        for e in range(n_exp):
            slot, col = down_place(b, e)
            down_dot(e, up_buf[slot, 0:ff, col:col + COLS])
        combine(b)

        @pl.when(b + RING < n_blk)
        def _():
            down_start(b + RING)

        stage_one(b - 1)

        @pl.when(b > 2)
        def _():
            stage_two(b - 3)
        return carry

    def finish(b, carry):
        landed(in_two.at[b], two_recv.at[b])
        col = pl.multiple_of(b * COLS, COLS)
        out_ref[:, pl.ds(col, HALF)] = (part_own[b, 0, 0, :, 0:HALF] + in_x1[b, 0] + in_two[b, 0]).astype(BF16)
        out_ref[:, pl.ds(col + HALF, HALF)] = (part_own[b, 0, 0, :, HALF:COLS] + in_y1[b, 0] + in_two[b, 1]).astype(BF16)
        return carry

    last = n_blk - 1

    def last_copy(rel):
        return remote(part_own.at[last, rel // 2, rel % 2], in_last.at[rel - 1],
                      last_sent, last_recv.at[0], dev(rel, False))

    down_first()
    lax.fori_loop(1, n_blk, down_step, 0)
    stage_two(last - 2)
    lax.fori_loop(0, last - 4, finish, 0)
    pair_copy(last).wait_recv()
    part_own[last] = part_own[last] + part_recv[last]
    for rel in (3, 1, 2):
        last_copy(rel).start()
    stage_two(last - 1)
    lax.fori_loop(last - 4, last, finish, 0)
    landed(in_last, last_recv.at[0])
    total = part_own[last, 0, 0] + in_last[0] + in_last[1] + in_last[2]
    out_ref[:, last * COLS:] = total.astype(BF16)

    left(slots.at[pl.ds(0, 7), pl.ds(0, tok)], tok_sent)
    left(in_x1.at[pl.ds(0, 7), 0], meta_sent)
    left(part_recv, pair_sent)
    left(part_own.at[pl.ds(0, last), 0], one_sent)
    left(in_x1.at[pl.ds(0, last)], two_sent)
    left(in_last, last_sent)


def solution(mesh):
    token_spec = P(('dp', 'ep'), None)
    expert_spec = P('ep', None, None)

    def local_layer(x_loc, ids_loc, gates_loc, w_up, w_down):
        tok, top_n = ids_loc.shape
        dim = x_loc.shape[1]
        n_exp, _, ff = w_up.shape
        cap = tok // 2
        pair = 2 * tok
        lanes_n = n_exp * 2 * cap
        n_blk = dim // COLS
        rows = 8 * cap
        dims = (tok, top_n, dim, ff, n_exp, cap)
        dma = pltpu.SemaphoreType.DMA
        hbm = pl.BlockSpec(memory_space=pl.ANY)
        return pl.pallas_call(
            functools.partial(moe_kernel, dims),
            out_shape=pltpu.VMEM((tok, dim), BF16),
            in_specs=[hbm] * 5,
            out_specs=pl.BlockSpec(memory_space=pltpu.VMEM),
            scratch_shapes=[
                pltpu.VMEM((UP_SLOTS, dim, ff), BF16),
                pltpu.VMEM((n_exp, ff, COLS), BF16),
                pltpu.VMEM((top_n, tok), jnp.int32),
                pltpu.VMEM((top_n, tok), F32),
                pltpu.VMEM((4, pair, dim), BF16),
                pltpu.VMEM((4, pair, 128), F32),
                pltpu.VMEM((4, pair, lanes_n), BF16),
                pltpu.VMEM((n_exp, rows, dim), BF16),
                pltpu.VMEM((EARLY, rows - 2 * cap, ff), F32),
                pltpu.VMEM((n_exp, rows, ff), BF16),
                pltpu.VMEM((4, 3 * pair, lanes_n), BF16),
                pltpu.VMEM((4, lanes_n, COLS), BF16),
                pltpu.VMEM((n_blk, 2, 2, tok, COLS), F32),
                pltpu.VMEM((n_blk, 2, 2, tok, COLS), F32),
                pltpu.VMEM((n_blk, 2, 2, tok, COLS), F32),
                pltpu.VMEM((n_blk, 2, tok, HALF), F32),
                pltpu.VMEM((n_blk, 2, tok, HALF), F32),
                pltpu.VMEM((n_blk, 2, tok, HALF), F32),
                pltpu.VMEM((3, tok, COLS), F32),
                dma((UP_SLOTS,)), dma((1,)), dma((RING,)), dma((3,)), dma((6,)), dma((3,)), dma((2,)),
                dma((2, CHUNKS)), dma((CHUNKS,)), dma((3, CHUNKS)), dma((n_blk,)), dma((n_blk, 2)), dma((n_blk,)), dma((1,)),
            ],
            compiler_params=pltpu.CompilerParams(
                collective_id=0, has_side_effects=True, vmem_limit_bytes=67043328 - 2 * tok * dim),
            name='moe_layer',
        )(x_loc, ids_loc.T, gates_loc.T, w_up, w_down)

    return jax.shard_map(local_layer, mesh=mesh, in_specs=(token_spec, token_spec, token_spec, expert_spec, expert_spec),
                         out_specs=token_spec, check_vma=False)
```

```python
import functools

import jax
import jax.numpy as jnp
from jax import lax
from jax.experimental import pallas as pl
from jax.experimental.pallas import tpu as pltpu
from jax.sharding import PartitionSpec as P

MESH = pl.DeviceIdType.MESH
F32 = jnp.float32
BF16 = jnp.bfloat16

UP_SLOTS = 6
EARLY = 4
RING = UP_SLOTS // 2
PER_SLOT = 5
COLS = 256
HALF = COLS // 2
CHUNKS = 4


def gelu(z):
    inner = 0.7978845608028654 * (z + 0.044715 * (z * z * z))
    return 0.5 * z * (1.0 + jnp.tanh(inner))


def moe_kernel(dims, x_hbm, ids_hbm, gates_hbm, up_hbm, down_hbm, out_ref,
               up_buf, first_buf, ids_v, gates_v, x_all, meta_all, one_hot, slots, acc, hidden, mix, expert_out,
               part_own, part_send, part_recv, in_x1, in_y1, in_two, in_last,
               up_sem, first_sem, down_sem, in_sem, send_sem, meta_recv, mpair_recv,
               tok_recv, diag_recv, tpair_recv, pair_recv, near_recv, one_recv, two_recv, last_recv, own_recv):
    tok, top_n, dim, ff, n_exp, cap = dims
    pair = 2 * tok
    per_exp = 2 * cap
    lanes_n = n_exp * per_exp
    n_blk = dim // COLS
    chunk = dim // CHUNKS
    dp = lax.axis_index('dp')
    me = lax.axis_index('ep')
    core = lax.rem(me, 2)
    chip = me // 2
    cx = lax.rem(chip, 2)
    cy = chip // 2

    def dev(rel, other_core):
        xx = 1 - cx if rel % 2 else cx
        yy = 1 - cy if rel // 2 else cy
        cc = 1 - core if other_core else core
        return (dp, (yy * 2 + xx) * 2 + cc)

    partner = dev(0, True)

    barrier = pltpu.get_barrier_semaphore()
    for rel in (3, 1, 2):
        pl.semaphore_signal(barrier, inc=1, device_id=dev(rel, False), device_id_type=MESH)
    pl.semaphore_signal(barrier, inc=1, device_id=partner, device_id_type=MESH)

    copy_x = pltpu.make_async_copy(x_hbm, x_all.at[0, pl.ds(0, tok)], in_sem.at[0])
    copy_ids = pltpu.make_async_copy(ids_hbm, ids_v, in_sem.at[1])
    copy_gates = pltpu.make_async_copy(gates_hbm, gates_v, in_sem.at[2])
    copy_x.start()
    copy_ids.start()
    copy_gates.start()

    def up_copy(e):
        slot = lax.rem(e, UP_SLOTS)
        return pltpu.make_async_copy(up_hbm.at[e], up_buf.at[slot], up_sem.at[slot])

    first_copy = pltpu.make_async_copy(down_hbm.at[:, :, pl.ds(0, COLS)], first_buf, first_sem.at[0])

    def down_place(b, e):
        return 2 * lax.rem(b, RING) + e // PER_SLOT, (e % PER_SLOT) * COLS

    def down_copy(b, e):
        slot, col = down_place(b, e)
        return pltpu.make_async_copy(
            down_hbm.at[e, :, pl.ds(pl.multiple_of(b * COLS, COLS), COLS)], up_buf.at[slot, pl.ds(0, ff), pl.ds(col, COLS)],
            down_sem.at[lax.rem(b, RING)])

    def down_start(b):
        for e in range(n_exp):
            down_copy(b, e).start()

    def down_wait(b):
        pltpu.make_async_copy(down_hbm.at[:, :, pl.ds(0, COLS)], first_buf, down_sem.at[lax.rem(b, RING)]).wait()

    copy_ids.wait()
    copy_gates.wait()
    copy_x.wait()
    for e in range(UP_SLOTS):
        up_copy(e).start()
    first_copy.start()

    def remote(src, dst, send, recv, to):
        return pltpu.make_async_remote_copy(
            src_ref=src, dst_ref=dst, send_sem=send, recv_sem=recv, device_id=to, device_id_type=MESH)

    meta_sent, tok_sent, pair_sent, one_sent, two_sent, last_sent = (send_sem.at[i] for i in range(6))

    def meta_out(rel):
        return remote(meta_all.at[0, pl.ds(0, tok)], meta_all.at[rel, pl.ds(0, tok)],
                      meta_sent, meta_recv.at[rel - 1], dev(rel, False))

    def meta_pair(rel):
        return remote(meta_all.at[rel, pl.ds(0, tok)], meta_all.at[rel, pl.ds(tok, tok)],
                      meta_sent, mpair_recv.at[min(rel, 1)], partner)

    def tok_out(rel, c):
        cols = pl.ds(c * chunk, chunk)
        return remote(x_all.at[0, pl.ds(0, tok), cols], x_all.at[rel, pl.ds(0, tok), cols],
                      tok_sent, tok_recv.at[c], dev(rel, False))

    def tok_diag(via, c):
        cols = pl.ds(c * chunk + (via - 1) * (chunk // 2), chunk // 2)
        return remote(x_all.at[via, pl.ds(0, tok), cols], x_all.at[3, pl.ds(0, tok), cols],
                      tok_sent, diag_recv.at[c], dev(3 - via, False))

    def tok_pair(rel, c):
        cols = pl.ds(c * chunk, chunk)
        return remote(x_all.at[rel, pl.ds(0, tok), cols], x_all.at[rel, pl.ds(tok, tok), cols],
                      tok_sent, tpair_recv.at[0 if rel == 3 else 1, c], partner)

    own_pair = remote(x_all.at[0, pl.ds(0, tok)], x_all.at[0, pl.ds(tok, tok)], tok_sent, own_recv.at[0], partner)

    def landed(ref, sem):
        remote(ref, ref, send_sem.at[0], sem, partner).wait_recv()

    def left(ref, sem):
        remote(ref, ref, sem, tpair_recv.at[0, 0], partner).wait_send()

    pl.semaphore_wait(barrier, 4)
    tok_out(1, 0).start()
    tok_out(2, 0).start()
    own_pair.start()

    sub = lax.broadcasted_iota(jnp.int32, (64, tok), 0)
    chosen = jnp.zeros((64, tok), F32)
    dense_gate = jnp.zeros((64, tok), F32)
    for j in range(top_n):
        same = sub == ids_v[j:j + 1, :]
        chosen = jnp.where(same, 1.0, chosen)
        dense_gate = jnp.where(same, gates_v[j:j + 1, :], dense_gate)
    row_i = lax.broadcasted_iota(jnp.int32, (tok, tok), 0)
    col_i = lax.broadcasted_iota(jnp.int32, (tok, tok), 1)
    before = jnp.where(row_i < col_i, 1.0, 0.0).astype(BF16)
    rank = jnp.dot(chosen.astype(BF16), before, preferred_element_type=F32)
    meta_t = jnp.concatenate([jnp.where(chosen > 0.5, rank, -1.0), dense_gate], axis=0)
    meta_all[0, 0:tok, :] = meta_t.T
    for rel in (3, 1, 2):
        meta_out(rel).start()
    meta_pair(0).start()
    for c in (1, 2):
        tok_out(1, c).start()
        tok_out(2, c).start()

    e_row = lax.broadcasted_iota(jnp.int32, (128, lanes_n), 0)
    e_col = lax.broadcasted_iota(jnp.int32, (128, lanes_n), 1)
    k_rank = (e_row - n_exp * me) * per_exp
    k_gate = k_rank - 64 * per_exp
    pick_rank = jnp.where((e_col >= k_rank) & (e_col < k_rank + per_exp), 1.0, 0.0).astype(BF16)
    pick_gate = jnp.where((e_col >= k_gate) & (e_col < k_gate + per_exp), 1.0, 0.0).astype(BF16)
    slot_f = lax.broadcasted_iota(jnp.int32, (pair, lanes_n), 1).astype(F32)
    tok_i = lax.broadcasted_iota(jnp.int32, (pair, lanes_n), 0)
    seg = jnp.floor((slot_f + 0.5) * (1.0 / cap))
    want = slot_f - cap * seg
    half = seg - 2.0 * jnp.floor((seg + 0.5) * 0.5)
    own_half = jnp.where(tok_i >= tok, 1.0, 0.0)
    want = jnp.where(half == own_half, want, -2.0)

    def masks(rels):
        if rels == (0,):
            meta_pair(0).wait_recv()
        else:
            landed(meta_all.at[pl.ds(1, 3), pl.ds(tok, tok)], mpair_recv.at[1])
        for rel in rels:
            meta = meta_all[rel]
            g1 = meta.astype(BF16)
            rest = meta - g1.astype(F32)
            g2 = rest.astype(BF16)
            g3 = (rest - g2.astype(F32)).astype(BF16)
            rank_e = jnp.dot(g1, pick_rank, preferred_element_type=F32)
            hit = rank_e == want
            for i, g in enumerate((g1, g2, g3)):
                g_e = jnp.dot(g, pick_gate, preferred_element_type=F32)
                mix[rel, i * pair:(i + 1) * pair, :] = jnp.where(hit, g_e, 0.0).astype(BF16)
            one_hot[rel] = jnp.where(hit, 1.0, 0.0).astype(BF16)

    def arrived(c):
        landed(x_all.at[pl.ds(1, 2), pl.ds(0, tok), pl.ds(c * chunk, chunk)], tok_recv.at[c])
        for via in (1, 2):
            tok_diag(via, c).start()
            tok_pair(via, c).start()

    def diag_arrived(c):
        cols = pl.ds(c * chunk, chunk)
        landed(x_all.at[3, pl.ds(0, tok), cols], diag_recv.at[c])
        tok_pair(3, c).start()

    def place(rels, cs):
        for c in cs:
            cols = pl.ds(c * chunk, chunk)
            if 0 in rels and c == 0:
                own_pair.wait_recv()
            if 1 in rels:
                landed(x_all.at[pl.ds(1, 2), pl.ds(tok, tok), cols], tpair_recv.at[1, c])
            if 3 in rels:
                landed(x_all.at[3, pl.ds(tok, tok), cols], tpair_recv.at[0, c])
        for c in cs:
            for rel in rels:
                rows = lax.dot_general(one_hot[rel], x_all[rel, :, c * chunk:(c + 1) * chunk],
                                       (((0,), (0,)), ((), ())), preferred_element_type=F32).astype(BF16)
                for e in range(n_exp):
                    slots[e, rel * per_exp:(rel + 1) * per_exp, c * chunk:(c + 1) * chunk] = (
                        rows[e * per_exp:(e + 1) * per_exp])

    def early(e):
        up_copy(e).wait()
        z = jnp.dot(slots[e, 0:per_exp, :], up_buf[e], preferred_element_type=F32)
        hidden[e, 0:per_exp, :] = gelu(z).astype(BF16)

    def late_dot(e, lo, hi):
        return jnp.dot(slots[e, per_exp:, lo:hi], up_buf[e, lo:hi, :], preferred_element_type=F32)

    def work_first():
        for e in range(EARLY):
            acc[e] = late_dot(e, 0, chunk)

    def work_second(e0, e1):
        for e in range(e0, e1):
            acc[e] = acc[e] + late_dot(e, chunk, 2 * chunk)

    def work_third(e0, e1):
        for e in range(e0, e1):
            hidden[e, per_exp:, :] = gelu(acc[e] + late_dot(e, 2 * chunk, dim)).astype(BF16)
        for e in range(e0, e1):
            if e + UP_SLOTS < n_exp:
                up_copy(e + UP_SLOTS).start()

    def work_whole(e0, e1):
        for e in range(e0, e1):
            up_copy(e).wait()
        for e in range(e0, e1):
            z = jnp.dot(slots[e], up_buf[e % UP_SLOTS], preferred_element_type=F32)
            hidden[e] = gelu(z).astype(BF16)

    masks((0,))
    place((0,), range(CHUNKS))
    early(0)
    arrived(0)
    tok_out(1, 3).start()
    tok_out(2, 3).start()
    early(1)
    for rel in (1, 2, 3):
        meta_out(rel).wait_recv()
        meta_pair(rel).start()
    arrived(1)
    early(2)
    arrived(2)
    masks((1, 2, 3))
    place((1, 2), (0,))
    diag_arrived(0)
    arrived(3)
    early(3)
    place((3,), (0,))
    diag_arrived(1)
    work_first()
    diag_arrived(2)
    place((1, 2, 3), (1,))
    work_second(0, 2)
    diag_arrived(3)
    work_second(2, 4)
    place((1, 2, 3), (2,))
    place((1, 2, 3), (3,))
    work_third(0, 2)
    work_third(2, 4)
    down_start(1)
    work_whole(4, 6)
    down_start(2)
    work_whole(6, 8)
    down_start(3)

    def pair_copy(b):
        return remote(part_send.at[b], part_recv.at[b], pair_sent, pair_recv.at[b], partner)

    lo, hi = pl.ds(0, HALF), pl.ds(HALF, HALF)
    everyone = pl.ds(0, 2)

    def first_x(b):
        return remote(part_own.at[b, everyone, 1, :, lo], in_x1.at[b], one_sent, one_recv.at[b, 0], dev(1, False))

    def first_y(b):
        return remote(part_own.at[b, 1, everyone, :, hi], in_y1.at[b], one_sent, one_recv.at[b, 1], dev(2, False))

    def second_y(b):
        return remote(part_own.at[b, 1, 0, :, lo], in_two.at[b, 0], two_sent, two_recv.at[b], dev(2, False))

    def second_x(b):
        return remote(part_own.at[b, 0, 1, :, hi], in_two.at[b, 1], two_sent, two_recv.at[b], dev(1, False))

    def stage_one(b):
        pair_copy(b).wait_recv()
        part_own[b] = part_own[b] + part_recv[b]
        first_x(b).start()
        first_y(b).start()

    def stage_two(b):
        first_x(b).wait_recv()
        part_own[b, 1, 0, :, 0:HALF] = part_own[b, 1, 0, :, 0:HALF] + in_x1[b, 1]
        second_y(b).start()
        first_y(b).wait_recv()
        part_own[b, 0, 1, :, HALF:COLS] = part_own[b, 0, 1, :, HALF:COLS] + in_y1[b, 1]
        second_x(b).start()

    def down_dot(e, weights, rels):
        first, count = rels[0] * per_exp, len(rels) * per_exp
        o = jnp.dot(hidden[e, first:first + count, :], weights, preferred_element_type=F32).astype(BF16)
        for i, rel in enumerate(rels):
            expert_out[rel, e * per_exp:(e + 1) * per_exp, :] = o[i * per_exp:(i + 1) * per_exp]

    def down_dots(b, rels):
        for e in range(n_exp):
            slot, col = down_place(b, e)
            down_dot(e, up_buf[slot, 0:ff, col:col + COLS], rels)

    def combine(b, rels):
        for rel in rels:
            y3 = jnp.dot(mix[rel], expert_out[rel], preferred_element_type=F32)
            y = y3[0:pair] + (y3[pair:2 * pair] + y3[2 * pair:3 * pair])
            part_own[b, rel // 2, rel % 2] = y[0:tok]
            part_send[b, rel // 2, rel % 2] = y[tok:pair]

    every, far, near = (0, 1, 2, 3), (1, 2, 3), (0,)

    def down_step(b, carry):
        down_wait(b)
        down_dots(b, every)
        combine(b, every)
        pair_copy(b).start()
        stage_one(b - 1)

        @pl.when(b > 2)
        def _():
            stage_two(b - 3)

        down_start(b + RING)
        return carry

    def far_part(b, i):
        where = (b, 0, 1) if i == 0 else (b, 1)
        return remote(part_send.at[where], part_recv.at[where], pair_sent, pair_recv.at[b], partner)

    def near_part(b):
        return remote(part_send.at[b, 0, 0], part_recv.at[b, 0, 0], pair_sent, near_recv.at[b - split], partner)

    def work_far(b):
        down_wait(b)
        down_dots(b, far)
        combine(b, far)
        far_part(b, 0).start()
        far_part(b, 1).start()

    def work_near(b):
        down_dots(b, near)
        combine(b, near)
        near_part(b).start()

    def add_far(b):
        landed(in_last, pair_recv.at[b])
        part_own[b, 0, 1] = part_own[b, 0, 1] + part_recv[b, 0, 1]
        part_own[b, 1] = part_own[b, 1] + part_recv[b, 1]

    def stage_far(b):
        add_far(b)
        first_x(b).start()
        first_y(b).start()

    def finish(b, carry):
        landed(in_two.at[b], two_recv.at[b])
        own = part_own[b, 0, 0]
        if not isinstance(b, jax.Array):
            near_part(b).wait_recv()
            own = own + part_recv[b, 0, 0]
        col = b * COLS if not isinstance(b, jax.Array) else pl.multiple_of(b * COLS, COLS)
        out_ref[:, pl.ds(col, HALF)] = (own[:, 0:HALF] + in_x1[b, 0] + in_two[b, 0]).astype(BF16)
        out_ref[:, pl.ds(col + HALF, HALF)] = (own[:, HALF:COLS] + in_y1[b, 0] + in_two[b, 1]).astype(BF16)
        return carry

    last = n_blk - 1
    split = n_blk - RING

    def last_copy(rel):
        return remote(part_own.at[last, rel // 2, rel % 2], in_last.at[rel - 1],
                      last_sent, last_recv.at[0], dev(rel, False))

    first_copy.wait()
    for e in range(n_exp):
        down_dot(e, first_buf[e], every)
    combine(0, every)
    pair_copy(0).start()
    lax.fori_loop(1, split, down_step, 0)
    work_far(split)
    stage_one(split - 1)
    stage_two(split - 3)
    work_far(split + 1)
    stage_far(split)
    stage_two(split - 2)
    work_far(split + 2)
    stage_far(split + 1)
    work_near(split)
    stage_two(split - 1)
    add_far(last)
    for rel in (3, 1, 2):
        last_copy(rel).start()
    work_near(split + 1)
    stage_two(split)
    work_near(split + 2)
    stage_two(split + 1)
    lax.fori_loop(0, split, finish, 0)
    finish(split, 0)
    finish(split + 1, 0)
    near_part(last).wait_recv()
    own_last = part_own[last, 0, 0] + part_recv[last, 0, 0]
    landed(in_last, last_recv.at[0])
    out_ref[:, last * COLS:] = (own_last + in_last[0] + in_last[1] + in_last[2]).astype(BF16)

    left(slots.at[pl.ds(0, 7), pl.ds(0, tok)], tok_sent)
    left(in_x1.at[pl.ds(0, 7), 0], meta_sent)
    left(part_recv, pair_sent)
    left(part_own.at[pl.ds(0, last), 0], one_sent)
    left(in_x1.at[pl.ds(0, last)], two_sent)
    left(in_last, last_sent)


def solution(mesh):
    token_spec = P(('dp', 'ep'), None)
    expert_spec = P('ep', None, None)

    def local_layer(x_loc, ids_loc, gates_loc, w_up, w_down):
        tok, top_n = ids_loc.shape
        dim = x_loc.shape[1]
        n_exp, _, ff = w_up.shape
        cap = tok // 2
        pair = 2 * tok
        lanes_n = n_exp * 2 * cap
        n_blk = dim // COLS
        rows = 8 * cap
        dims = (tok, top_n, dim, ff, n_exp, cap)
        dma = pltpu.SemaphoreType.DMA
        hbm = pl.BlockSpec(memory_space=pl.ANY)
        return pl.pallas_call(
            functools.partial(moe_kernel, dims),
            out_shape=pltpu.VMEM((tok, dim), BF16),
            in_specs=[hbm] * 5,
            out_specs=pl.BlockSpec(memory_space=pltpu.VMEM),
            scratch_shapes=[
                pltpu.VMEM((UP_SLOTS, dim, ff), BF16),
                pltpu.VMEM((n_exp, ff, COLS), BF16),
                pltpu.VMEM((top_n, tok), jnp.int32),
                pltpu.VMEM((top_n, tok), F32),
                pltpu.VMEM((4, pair, dim), BF16),
                pltpu.VMEM((4, pair, 128), F32),
                pltpu.VMEM((4, pair, lanes_n), BF16),
                pltpu.VMEM((n_exp, rows, dim), BF16),
                pltpu.VMEM((EARLY, rows - 2 * cap, ff), F32),
                pltpu.VMEM((n_exp, rows, ff), BF16),
                pltpu.VMEM((4, 3 * pair, lanes_n), BF16),
                pltpu.VMEM((4, lanes_n, COLS), BF16),
                pltpu.VMEM((n_blk, 2, 2, tok, COLS), F32),
                pltpu.VMEM((n_blk, 2, 2, tok, COLS), F32),
                pltpu.VMEM((n_blk, 2, 2, tok, COLS), F32),
                pltpu.VMEM((n_blk, 2, tok, HALF), F32),
                pltpu.VMEM((n_blk, 2, tok, HALF), F32),
                pltpu.VMEM((n_blk, 2, tok, HALF), F32),
                pltpu.VMEM((3, tok, COLS), F32),
                dma((UP_SLOTS,)), dma((1,)), dma((RING,)), dma((3,)), dma((6,)), dma((3,)), dma((2,)),
                dma((CHUNKS,)), dma((CHUNKS,)), dma((2, CHUNKS)), dma((n_blk,)), dma((RING,)), dma((n_blk - 1, 2)), dma((n_blk - 1,)), dma((1,)), dma((1,)),
            ],
            compiler_params=pltpu.CompilerParams(
                collective_id=0, has_side_effects=True, vmem_limit_bytes=67043328 - 2 * tok * dim),
            name='moe_layer',
        )(x_loc, ids_loc.T, gates_loc.T, w_up, w_down)

    return jax.shard_map(local_layer, mesh=mesh, in_specs=(token_spec, token_spec, token_spec, expert_spec, expert_spec),
                         out_specs=token_spec, check_vma=False)
```

```python
import functools

import jax
import jax.numpy as jnp
from jax import lax
from jax.experimental import pallas as pl
from jax.experimental.pallas import tpu as pltpu
from jax.sharding import PartitionSpec as P

MESH = pl.DeviceIdType.MESH
F32 = jnp.float32
BF16 = jnp.bfloat16

UP_SLOTS = 6
EARLY = 4
RING = UP_SLOTS // 2
PER_SLOT = 5
COLS = 256
HALF = COLS // 2
CHUNKS = 4


def gelu(z):
    inner = 0.7978845608028654 * (z + 0.044715 * (z * z * z))
    return 0.5 * z * (1.0 + jnp.tanh(inner))


def moe_kernel(dims, x_hbm, ids_hbm, gates_hbm, up_hbm, down_hbm, out_ref,
               up_buf, first_buf, ids_v, gates_v, x_all, meta_all, one_hot, slots, acc, hidden, mix, expert_out,
               part_own, part_send, part_recv, in_x1, in_y1, in_two, in_last,
               up_sem, first_sem, down_sem, in_sem, send_sem, meta_recv, mpair_recv,
               tok_recv, diag_recv, tpair_recv, pair_recv, near_recv, one_recv, two_recv, last_recv, own_recv):
    tok, top_n, dim, ff, n_exp, cap = dims
    pair = 2 * tok
    per_exp = 2 * cap
    lanes_n = n_exp * per_exp
    n_blk = dim // COLS
    chunk = dim // CHUNKS
    dp = lax.axis_index('dp')
    me = lax.axis_index('ep')
    core = lax.rem(me, 2)
    chip = me // 2
    cx = lax.rem(chip, 2)
    cy = chip // 2

    def dev(rel, other_core):
        xx = 1 - cx if rel % 2 else cx
        yy = 1 - cy if rel // 2 else cy
        cc = 1 - core if other_core else core
        return (dp, (yy * 2 + xx) * 2 + cc)

    partner = dev(0, True)

    barrier = pltpu.get_barrier_semaphore()
    for rel in (3, 1, 2):
        pl.semaphore_signal(barrier, inc=1, device_id=dev(rel, False), device_id_type=MESH)
    pl.semaphore_signal(barrier, inc=1, device_id=partner, device_id_type=MESH)

    copy_x = pltpu.make_async_copy(x_hbm, x_all.at[0, pl.ds(0, tok)], in_sem.at[0])
    copy_ids = pltpu.make_async_copy(ids_hbm, ids_v, in_sem.at[1])
    copy_gates = pltpu.make_async_copy(gates_hbm, gates_v, in_sem.at[2])
    copy_x.start()
    copy_ids.start()
    copy_gates.start()

    def up_copy(e):
        slot = lax.rem(e, UP_SLOTS)
        return pltpu.make_async_copy(up_hbm.at[e], up_buf.at[slot], up_sem.at[slot])

    first_copy = pltpu.make_async_copy(down_hbm.at[:, :, pl.ds(0, COLS)], first_buf, first_sem.at[0])

    def down_place(b, e):
        return 2 * lax.rem(b, RING) + e // PER_SLOT, (e % PER_SLOT) * COLS

    def down_copy(b, e):
        slot, col = down_place(b, e)
        return pltpu.make_async_copy(
            down_hbm.at[e, :, pl.ds(pl.multiple_of(b * COLS, COLS), COLS)], up_buf.at[slot, pl.ds(0, ff), pl.ds(col, COLS)],
            down_sem.at[lax.rem(b, RING)])

    def down_start(b):
        for e in range(n_exp):
            down_copy(b, e).start()

    def down_wait(b):
        pltpu.make_async_copy(down_hbm.at[:, :, pl.ds(0, COLS)], first_buf, down_sem.at[lax.rem(b, RING)]).wait()

    copy_ids.wait()
    copy_gates.wait()
    copy_x.wait()
    for e in range(UP_SLOTS):
        up_copy(e).start()
    first_copy.start()

    def remote(src, dst, send, recv, to):
        return pltpu.make_async_remote_copy(
            src_ref=src, dst_ref=dst, send_sem=send, recv_sem=recv, device_id=to, device_id_type=MESH)

    meta_sent, tok_sent, pair_sent, one_sent, two_sent, last_sent = (send_sem.at[i] for i in range(6))

    def meta_out(rel):
        return remote(meta_all.at[0, pl.ds(0, tok)], meta_all.at[rel, pl.ds(0, tok)],
                      meta_sent, meta_recv.at[rel - 1], dev(rel, False))

    def meta_pair(rel):
        return remote(meta_all.at[rel, pl.ds(0, tok)], meta_all.at[rel, pl.ds(tok, tok)],
                      meta_sent, mpair_recv.at[min(rel, 1)], partner)

    def tok_out(rel, c):
        cols = pl.ds(c * chunk, chunk)
        return remote(x_all.at[0, pl.ds(0, tok), cols], x_all.at[rel, pl.ds(0, tok), cols],
                      tok_sent, tok_recv.at[c], dev(rel, False))

    def tok_diag(via, c):
        cols = pl.ds(c * chunk + (via - 1) * (chunk // 2), chunk // 2)
        return remote(x_all.at[via, pl.ds(0, tok), cols], x_all.at[3, pl.ds(0, tok), cols],
                      tok_sent, diag_recv.at[c], dev(3 - via, False))

    def tok_pair(rel, c):
        cols = pl.ds(c * chunk, chunk)
        return remote(x_all.at[rel, pl.ds(0, tok), cols], x_all.at[rel, pl.ds(tok, tok), cols],
                      tok_sent, tpair_recv.at[0 if rel == 3 else 1, c], partner)

    own_pair = remote(x_all.at[0, pl.ds(0, tok)], x_all.at[0, pl.ds(tok, tok)], tok_sent, own_recv.at[0], partner)

    def landed(ref, sem):
        remote(ref, ref, send_sem.at[0], sem, partner).wait_recv()

    def left(ref, sem):
        remote(ref, ref, sem, tpair_recv.at[0, 0], partner).wait_send()

    pl.semaphore_wait(barrier, 4)
    tok_out(1, 0).start()
    tok_out(2, 0).start()
    own_pair.start()

    sub = lax.broadcasted_iota(jnp.int32, (64, tok), 0)
    chosen = jnp.zeros((64, tok), F32)
    dense_gate = jnp.zeros((64, tok), F32)
    for j in range(top_n):
        same = sub == ids_v[j:j + 1, :]
        chosen = jnp.where(same, 1.0, chosen)
        dense_gate = jnp.where(same, gates_v[j:j + 1, :], dense_gate)
    row_i = lax.broadcasted_iota(jnp.int32, (tok, tok), 0)
    col_i = lax.broadcasted_iota(jnp.int32, (tok, tok), 1)
    before = jnp.where(row_i < col_i, 1.0, 0.0).astype(BF16)
    rank = jnp.dot(chosen.astype(BF16), before, preferred_element_type=F32)
    meta_t = jnp.concatenate([jnp.where(chosen > 0.5, rank, -1.0), dense_gate], axis=0)
    meta_all[0, 0:tok, :] = meta_t.T
    for rel in (3, 1, 2):
        meta_out(rel).start()
    meta_pair(0).start()
    for c in (1, 2):
        tok_out(1, c).start()
        tok_out(2, c).start()

    e_row = lax.broadcasted_iota(jnp.int32, (128, lanes_n), 0)
    e_col = lax.broadcasted_iota(jnp.int32, (128, lanes_n), 1)
    k_rank = (e_row - n_exp * me) * per_exp
    k_gate = k_rank - 64 * per_exp
    pick_rank = jnp.where((e_col >= k_rank) & (e_col < k_rank + per_exp), 1.0, 0.0).astype(BF16)
    pick_gate = jnp.where((e_col >= k_gate) & (e_col < k_gate + per_exp), 1.0, 0.0).astype(BF16)
    slot_f = lax.broadcasted_iota(jnp.int32, (pair, lanes_n), 1).astype(F32)
    tok_i = lax.broadcasted_iota(jnp.int32, (pair, lanes_n), 0)
    seg = jnp.floor((slot_f + 0.5) * (1.0 / cap))
    want = slot_f - cap * seg
    half = seg - 2.0 * jnp.floor((seg + 0.5) * 0.5)
    own_half = jnp.where(tok_i >= tok, 1.0, 0.0)
    want = jnp.where(half == own_half, want, -2.0)

    def masks(rels):
        if rels == (0,):
            meta_pair(0).wait_recv()
        else:
            landed(meta_all.at[pl.ds(1, 3), pl.ds(tok, tok)], mpair_recv.at[1])
        for rel in rels:
            meta = meta_all[rel]
            g1 = meta.astype(BF16)
            rest = meta - g1.astype(F32)
            g2 = rest.astype(BF16)
            g3 = (rest - g2.astype(F32)).astype(BF16)
            rank_e = jnp.dot(g1, pick_rank, preferred_element_type=F32)
            hit = rank_e == want
            for i, g in enumerate((g1, g2, g3)):
                g_e = jnp.dot(g, pick_gate, preferred_element_type=F32)
                mix[rel, i * pair:(i + 1) * pair, :] = jnp.where(hit, g_e, 0.0).astype(BF16)
            one_hot[rel] = jnp.where(hit, 1.0, 0.0).astype(BF16)

    def arrived(c):
        landed(x_all.at[pl.ds(1, 2), pl.ds(0, tok), pl.ds(c * chunk, chunk)], tok_recv.at[c])
        for via in (1, 2):
            tok_diag(via, c).start()
            tok_pair(via, c).start()

    def diag_arrived(c):
        cols = pl.ds(c * chunk, chunk)
        landed(x_all.at[3, pl.ds(0, tok), cols], diag_recv.at[c])
        tok_pair(3, c).start()

    def place(rels, cs):
        for c in cs:
            cols = pl.ds(c * chunk, chunk)
            if 0 in rels and c == 0:
                own_pair.wait_recv()
            if 1 in rels:
                landed(x_all.at[pl.ds(1, 2), pl.ds(tok, tok), cols], tpair_recv.at[1, c])
            if 3 in rels:
                landed(x_all.at[3, pl.ds(tok, tok), cols], tpair_recv.at[0, c])
        for c in cs:
            for rel in rels:
                rows = lax.dot_general(one_hot[rel], x_all[rel, :, c * chunk:(c + 1) * chunk],
                                       (((0,), (0,)), ((), ())), preferred_element_type=F32).astype(BF16)
                for e in range(n_exp):
                    slots[e, rel * per_exp:(rel + 1) * per_exp, c * chunk:(c + 1) * chunk] = (
                        rows[e * per_exp:(e + 1) * per_exp])

    def early(e):
        up_copy(e).wait()
        z = jnp.dot(slots[e, 0:per_exp, :], up_buf[e], preferred_element_type=F32)
        hidden[e, 0:per_exp, :] = gelu(z).astype(BF16)

    def late_dot(e, lo, hi):
        return jnp.dot(slots[e, per_exp:, lo:hi], up_buf[e, lo:hi, :], preferred_element_type=F32)

    def work_first():
        for e in range(EARLY):
            acc[e] = late_dot(e, 0, chunk)

    def work_second(e0, e1):
        for e in range(e0, e1):
            acc[e] = acc[e] + late_dot(e, chunk, 2 * chunk)

    def work_third(e0, e1):
        for e in range(e0, e1):
            hidden[e, per_exp:, :] = gelu(acc[e] + late_dot(e, 2 * chunk, dim)).astype(BF16)
        for e in range(e0, e1):
            if e + UP_SLOTS < n_exp:
                up_copy(e + UP_SLOTS).start()

    def work_whole(e0, e1):
        for e in range(e0, e1):
            up_copy(e).wait()
        for e in range(e0, e1):
            z = jnp.dot(slots[e], up_buf[e % UP_SLOTS], preferred_element_type=F32)
            hidden[e] = gelu(z).astype(BF16)

    masks((0,))
    place((0,), range(CHUNKS))
    early(0)
    arrived(0)
    tok_out(1, 3).start()
    tok_out(2, 3).start()
    early(1)
    for rel in (1, 2, 3):
        meta_out(rel).wait_recv()
        meta_pair(rel).start()
    arrived(1)
    early(2)
    arrived(2)
    masks((1, 2, 3))
    place((1, 2), (0,))
    diag_arrived(0)
    arrived(3)
    early(3)
    place((3,), (0,))
    diag_arrived(1)
    work_first()
    diag_arrived(2)
    place((1, 2, 3), (1,))
    work_second(0, 2)
    diag_arrived(3)
    work_second(2, 4)
    place((1, 2, 3), (2,))
    place((1, 2, 3), (3,))
    work_third(0, 2)
    work_third(2, 4)
    down_start(1)
    work_whole(4, 6)
    down_start(2)
    work_whole(6, 8)
    down_start(3)

    def pair_copy(b):
        return remote(part_send.at[b], part_recv.at[b], pair_sent, pair_recv.at[b], partner)

    lo, hi = pl.ds(0, HALF), pl.ds(HALF, HALF)
    everyone = pl.ds(0, 2)

    def first_x(b):
        return remote(part_own.at[b, everyone, 1, :, lo], in_x1.at[b], one_sent, one_recv.at[b], dev(1, False))

    def first_y(b):
        return remote(part_own.at[b, 1, everyone, :, hi], in_y1.at[b], one_sent, one_recv.at[b], dev(2, False))

    def second_y(b):
        return remote(part_own.at[b, 1, 0, :, lo], in_two.at[b, 0], two_sent, two_recv.at[b], dev(2, False))

    def second_x(b):
        return remote(part_own.at[b, 0, 1, :, hi], in_two.at[b, 1], two_sent, two_recv.at[b], dev(1, False))

    def stage_one(b):
        pair_copy(b).wait_recv()
        part_own[b] = part_own[b] + part_recv[b]
        first_x(b).start()
        first_y(b).start()

    def stage_two(b):
        landed(in_x1.at[pl.ds(0, 2)], one_recv.at[b])
        part_own[b, 1, 0, :, 0:HALF] = part_own[b, 1, 0, :, 0:HALF] + in_x1[b, 1]
        second_y(b).start()
        part_own[b, 0, 1, :, HALF:COLS] = part_own[b, 0, 1, :, HALF:COLS] + in_y1[b, 1]
        second_x(b).start()

    def down_dot(e, weights, rels):
        first, count = rels[0] * per_exp, len(rels) * per_exp
        o = jnp.dot(hidden[e, first:first + count, :], weights, preferred_element_type=F32).astype(BF16)
        for i, rel in enumerate(rels):
            expert_out[rel, e * per_exp:(e + 1) * per_exp, :] = o[i * per_exp:(i + 1) * per_exp]

    def down_dots(b, rels):
        for e in range(n_exp):
            slot, col = down_place(b, e)
            down_dot(e, up_buf[slot, 0:ff, col:col + COLS], rels)

    def combine(b, rels):
        for rel in rels:
            y3 = jnp.dot(mix[rel], expert_out[rel], preferred_element_type=F32)
            y = y3[0:pair] + (y3[pair:2 * pair] + y3[2 * pair:3 * pair])
            part_own[b, rel // 2, rel % 2] = y[0:tok]
            part_send[b, rel // 2, rel % 2] = y[tok:pair]

    every, far, near = (0, 1, 2, 3), (1, 2, 3), (0,)

    def down_step(b, carry):
        down_wait(b)
        down_dots(b, every)
        combine(b, every)
        pair_copy(b).start()
        stage_one(b - 1)

        @pl.when(b > 2)
        def _():
            stage_two(b - 3)

        down_start(b + RING)
        return carry

    def far_part(b, i):
        where = (b, 0, 1) if i == 0 else (b, 1)
        return remote(part_send.at[where], part_recv.at[where], pair_sent, pair_recv.at[b], partner)

    def near_part(b):
        return remote(part_send.at[b, 0, 0], part_recv.at[b, 0, 0], pair_sent, near_recv.at[b - split], partner)

    def work_far(b):
        down_wait(b)
        down_dots(b, far)
        combine(b, far)
        far_part(b, 0).start()
        far_part(b, 1).start()

    def work_near(b):
        down_dots(b, near)
        combine(b, near)
        near_part(b).start()

    def add_far(b):
        landed(in_last, pair_recv.at[b])
        part_own[b, 0, 1] = part_own[b, 0, 1] + part_recv[b, 0, 1]
        part_own[b, 1] = part_own[b, 1] + part_recv[b, 1]

    def stage_far(b):
        add_far(b)
        first_x(b).start()
        first_y(b).start()

    def finish(b, carry):
        landed(in_two.at[b], two_recv.at[b])
        own = part_own[b, 0, 0]
        if not isinstance(b, jax.Array):
            near_part(b).wait_recv()
            own = own + part_recv[b, 0, 0]
        col = b * COLS if not isinstance(b, jax.Array) else pl.multiple_of(b * COLS, COLS)
        out_ref[:, pl.ds(col, HALF)] = (own[:, 0:HALF] + in_x1[b, 0] + in_two[b, 0]).astype(BF16)
        out_ref[:, pl.ds(col + HALF, HALF)] = (own[:, HALF:COLS] + in_y1[b, 0] + in_two[b, 1]).astype(BF16)
        return carry

    last = n_blk - 1
    split = n_blk - RING

    def last_copy(rel):
        return remote(part_own.at[last, rel // 2, rel % 2], in_last.at[rel - 1],
                      last_sent, last_recv.at[0], dev(rel, False))

    first_copy.wait()
    for e in range(n_exp):
        down_dot(e, first_buf[e], every)
    combine(0, every)
    pair_copy(0).start()
    lax.fori_loop(1, split, down_step, 0)
    work_far(split)
    stage_one(split - 1)
    stage_two(split - 3)
    work_far(split + 1)
    stage_far(split)
    stage_two(split - 2)
    work_far(split + 2)
    stage_far(split + 1)
    work_near(split)
    stage_two(split - 1)
    add_far(last)
    for rel in (3, 1, 2):
        last_copy(rel).start()
    work_near(split + 1)
    stage_two(split)
    work_near(split + 2)
    stage_two(split + 1)
    lax.fori_loop(0, split, finish, 0)
    finish(split, 0)
    finish(split + 1, 0)
    near_part(last).wait_recv()
    own_last = part_own[last, 0, 0] + part_recv[last, 0, 0]
    landed(in_last, last_recv.at[0])
    out_ref[:, last * COLS:] = (own_last + in_last[0] + in_last[1] + in_last[2]).astype(BF16)

    left(slots.at[pl.ds(0, 7), pl.ds(0, tok)], tok_sent)
    left(in_x1.at[pl.ds(0, 7), 0], meta_sent)
    left(part_recv, pair_sent)
    left(part_own.at[pl.ds(0, last), 0], one_sent)
    left(in_x1.at[pl.ds(0, last)], two_sent)
    left(in_last, last_sent)


def solution(mesh):
    token_spec = P(('dp', 'ep'), None)
    expert_spec = P('ep', None, None)

    def local_layer(x_loc, ids_loc, gates_loc, w_up, w_down):
        tok, top_n = ids_loc.shape
        dim = x_loc.shape[1]
        n_exp, _, ff = w_up.shape
        cap = tok // 2
        pair = 2 * tok
        lanes_n = n_exp * 2 * cap
        n_blk = dim // COLS
        rows = 8 * cap
        dims = (tok, top_n, dim, ff, n_exp, cap)
        dma = pltpu.SemaphoreType.DMA
        hbm = pl.BlockSpec(memory_space=pl.ANY)
        return pl.pallas_call(
            functools.partial(moe_kernel, dims),
            out_shape=pltpu.VMEM((tok, dim), BF16),
            in_specs=[hbm] * 5,
            out_specs=pl.BlockSpec(memory_space=pltpu.VMEM),
            scratch_shapes=[
                pltpu.VMEM((UP_SLOTS, dim, ff), BF16),
                pltpu.VMEM((n_exp, ff, COLS), BF16),
                pltpu.VMEM((top_n, tok), jnp.int32),
                pltpu.VMEM((top_n, tok), F32),
                pltpu.VMEM((4, pair, dim), BF16),
                pltpu.VMEM((4, pair, 128), F32),
                pltpu.VMEM((4, pair, lanes_n), BF16),
                pltpu.VMEM((n_exp, rows, dim), BF16),
                pltpu.VMEM((EARLY, rows - 2 * cap, ff), F32),
                pltpu.VMEM((n_exp, rows, ff), BF16),
                pltpu.VMEM((4, 3 * pair, lanes_n), BF16),
                pltpu.VMEM((4, lanes_n, COLS), BF16),
                pltpu.VMEM((n_blk, 2, 2, tok, COLS), F32),
                pltpu.VMEM((n_blk, 2, 2, tok, COLS), F32),
                pltpu.VMEM((n_blk, 2, 2, tok, COLS), F32),
                pltpu.VMEM((n_blk, 2, tok, HALF), F32),
                pltpu.VMEM((n_blk, 2, tok, HALF), F32),
                pltpu.VMEM((n_blk, 2, tok, HALF), F32),
                pltpu.VMEM((3, tok, COLS), F32),
                dma((UP_SLOTS,)), dma((1,)), dma((RING,)), dma((3,)), dma((6,)), dma((3,)), dma((2,)),
                dma((CHUNKS,)), dma((CHUNKS,)), dma((2, CHUNKS)), dma((n_blk,)), dma((RING,)), dma((n_blk - 1,)), dma((n_blk - 1,)), dma((1,)), dma((1,)),
            ],
            compiler_params=pltpu.CompilerParams(
                collective_id=0, has_side_effects=True, vmem_limit_bytes=67043328 - 2 * tok * dim),
            name='moe_layer',
        )(x_loc, ids_loc.T, gates_loc.T, w_up, w_down)

    return jax.shard_map(local_layer, mesh=mesh, in_specs=(token_spec, token_spec, token_spec, expert_spec, expert_spec),
                         out_specs=token_spec, check_vma=False)
```
